32 devices in a mesh: gx: 2 (over x), gy: 4 (over z), gz: 4 (over y, core).
Axes of the slice: x: 2, y: 2, z: 4, core: 2. Of those that a mesh axis runs over, the one named last changes fastest.
Arguments:
- fields: bfloat16 [7, 16, 32, 64], P(None, 'gx', 'gy', 'gz'), may hold values from -6 to 6
- grain_ids: int32 [16, 32, 64], P('gx', 'gy', 'gz'), may hold values from 0 to 127
- material_table: bfloat16 [128, 64], replicated, may hold values from -6 to 6
- input_weight: bfloat16 [64, 7], replicated, may hold values from -2 to 2
- kernel_fine: bfloat16 [64, 1728], replicated, may hold values from -0.15625 to 0.15625
- kernel_down: bfloat16 [128, 1728], replicated, may hold values from -0.15625 to 0.15625
- kernel_bottle: bfloat16 [256, 3456], P('gx'), may hold values from -0.109375 to 0.109375
- cotangent: bfloat16 [256, 8, 16, 32], P('gx', None, 'gy', 'gz'), may hold values from -6 to 6
Outputs:
- bottle: bfloat16 [256, 8, 16, 32], P('gx', None, 'gy', 'gz')
- grad_down: float32 [128, 1728], P('gx', ('gy', 'gz'))
- grad_bottle: float32 [256, 3456], P('gx', ('gy', 'gz'))
The draws below stay inside these ranges and needn't reach their ends.
Inputs may be any that keep to these rules, and one draw needn't show every extreme that they name: `grain_ids`: each voxel's grain, a row of material_table.
All inputs are finite; a program needn't handle non-finite values.
Results may differ from the reference program's by a relative error of at most 0.028.
Values may be sent and summed in bfloat16 or wider, within the bound.
No kernel may reach another device: no remote copies, remote signals or barrier semaphores. Data moves between devices by JAX's collectives and lax.ppermute only.
A program may use at most 64 MiB of HBM per device.

```python
import math
import jax
import jax.numpy as jnp
from jax import lax

C1 = 64
C2 = 128
C3 = 256
CF = 7
GRAINS = 128
TAPS = 27
NX = 16
NY = 32
NZ = 64
X1 = 8
Y1 = 16
Z1 = 32


def plant(drawn, rng, least, largest):
    longest = drawn.shape.index(max(drawn.shape))
    spots = []
    for shift in (0, 1):
        where = [jax.random.randint(jax.random.fold_in(rng, axis), (), 0, length) for axis, length in enumerate(drawn.shape)]
        where[longest] = (where[longest] + shift) % drawn.shape[longest]
        spots.append(tuple(where))
    return drawn.at[spots[0]].set(least).at[spots[1]].set(largest)


def block_levels(rng, extent, cuts, least, largest):
    level = 1.0
    for position, shards_of in cuts:
        draws = jax.random.uniform(jax.random.fold_in(jax.random.fold_in(rng, 6), position), (shards_of,), jnp.float32, least / len(cuts), largest / len(cuts))
        level = level * jnp.repeat(jnp.exp(draws), extent[position] // shards_of).reshape((-1,) + (1,) * (len(extent) - 1 - position))
    return level


def scatter_about(stream_key, dims, deviation, limit, split=(), held_as=jnp.bfloat16):
    drawn = deviation * jax.random.normal(stream_key, dims, jnp.float32)
    if split:
        drawn = drawn * block_levels(stream_key, dims, split, -0.22, 0.18)
    return jnp.clip(drawn, -limit, limit).astype(held_as)


def setup_inputs(seed: int = 0) -> dict:
    streams_of = jax.random.split(jax.random.key(seed), 9)
    return {
        "fields": scatter_about(streams_of[0], (CF, NX, NY, NZ), 1.0, 6.0, ((1, 2), (2, 4), (3, 4))),
        "grain_ids": plant(jax.random.randint(streams_of[1], (NX, NY, NZ), 0, GRAINS), jax.random.fold_in(streams_of[1], 1), 0, GRAINS - 1).astype(jnp.int32),
        "material_table": scatter_about(streams_of[2], (GRAINS, C1), 1.0, 6.0),
        "input_weight": scatter_about(streams_of[3], (C1, CF), CF ** -0.5, 2.0),
        "kernel_fine": scatter_about(streams_of[4], (C1, TAPS * C1), (TAPS * C1) ** -0.5, 0.15625),
        "kernel_down": scatter_about(streams_of[5], (C2, TAPS * C1), (TAPS * C1) ** -0.5, 0.15625),
        "kernel_bottle": scatter_about(streams_of[6], (C3, TAPS * C2), (TAPS * C2) ** -0.5, 0.109375, ((0, 2),)),
        "cotangent": scatter_about(streams_of[7], (C3, X1, Y1, Z1), 1.0, 6.0, ((0, 2), (2, 4), (3, 4))),
    }


def convolve(volume, kernel, stride):
    out_chans = kernel.shape[0]
    in_chans = kernel.shape[1] // 27
    weights = kernel.astype(jnp.float32).reshape(out_chans, 3, 3, 3, in_chans).transpose(0, 4, 1, 2, 3)
    result = lax.conv_general_dilated(volume.astype(jnp.float32)[None], weights, (stride, stride, stride), [(1, 1), (1, 1), (1, 1)], dimension_numbers=('NCDHW', 'OIDHW', 'NCDHW'), precision=lax.Precision.HIGHEST)
    return result[0]

def silu_grad(values):
    sigmoid = jax.nn.sigmoid(values)
    return sigmoid * (1.0 + values * (1.0 - sigmoid))

def reference(fields, grain_ids, material_table, input_weight, kernel_fine, kernel_down, kernel_bottle, cotangent):
    material = jnp.moveaxis(jnp.take(material_table, grain_ids, axis=0), 3, 0)
    mixture = jnp.dot(input_weight, fields.reshape(CF, -1), preferred_element_type=jnp.float32).reshape(material.shape) + material.astype(jnp.float32)
    embedded = jax.nn.silu(mixture).astype(jnp.bfloat16)
    fine = jax.nn.silu(convolve(embedded, kernel_fine, 1)).astype(jnp.bfloat16)
    pre_down = convolve(fine, kernel_down, 2)
    coarse = jax.nn.silu(pre_down).astype(jnp.bfloat16)

    def bottle_conv(volume, kernel):
        return convolve(volume, kernel, 1)
    pre_bottle, bottle_pull = jax.vjp(bottle_conv, coarse.astype(jnp.float32), kernel_bottle.astype(jnp.float32))
    bottle = jax.nn.silu(pre_bottle).astype(jnp.bfloat16)
    grad_pre_bottle = (cotangent.astype(jnp.float32) * silu_grad(pre_bottle)).astype(jnp.bfloat16)
    grad_down_act, grad_bottle = bottle_pull(grad_pre_bottle.astype(jnp.float32))
    grad_pre_down = (grad_down_act * silu_grad(pre_down)).astype(jnp.bfloat16)

    def down_conv(kernel):
        return convolve(fine, kernel, 2)
    ignored, down_pull = jax.vjp(down_conv, kernel_down.astype(jnp.float32))
    grad_down = down_pull(grad_pre_down.astype(jnp.float32))[0]
    grad_scale = 1.0 / math.sqrt(X1 * Y1 * Z1)
    return (bottle, grad_down * grad_scale, grad_bottle * grad_scale)
```

```python
import math

import jax
import jax.numpy as jnp
from jax import lax
from jax.experimental import pallas as pl
from jax.experimental.pallas import tpu as pltpu
from jax.sharding import PartitionSpec as P

F32 = jnp.float32
BF16 = jnp.bfloat16
CONTRACT_LANES = (((1,), (1,)), ((), ()))
CONTRACT_PLAIN = (((1,), (0,)), ((), ()))
TAPS_XY = [(kx, ky) for kx in range(3) for ky in range(3)]


def silu(values):
    return values / (1.0 + jnp.exp(-values))


def silu_grad(values):
    sigmoid = 1.0 / (1.0 + jnp.exp(-values))
    return sigmoid * (1.0 + values * (1.0 - sigmoid))


def flat(values):
    return values.reshape(-1, values.shape[-1])


def next_row(values):
    return pltpu.roll(values, values.shape[0] - 1, 0)


def previous_row(values):
    return pltpu.roll(values, 1, 0)


def shift_rows(values, forward):
    rows = flat(values)
    return (next_row(rows) if forward else previous_row(rows)).reshape(values.shape)


def forward_kernel(
    place, feat, wide_weight, wide_table, band_fine, band_down, kernel_bottle, cotangent,
    bottle_out, act_out, grad_out, fine_out, slope_out,
    emb, fine, coarse, grads, pre, fine_mask, coarse_mask, *, dims,
):
    nx, by, bz, c1, c2, outs, grains, limits = dims
    total_y, total_z = limits
    ny_emb, ny_fine, ny_mid, ny_bot, ny_own = by + 11, by + 9, by // 2 + 4, by // 2 + 2, by // 2
    quad = feat.shape[1] // 4
    nq = emb.shape[2]
    coarse_x = nx // 2
    own_x = slope_out.shape[0] // (ny_own * nq)
    lanes = 4 * c1
    half = lanes // 2

    shape = (ny_fine * nq, lanes)
    row = lax.broadcasted_iota(jnp.int32, shape, 0)
    lane = lax.broadcasted_iota(jnp.int32, shape, 1)
    y = place[0] * by - 5 + row // nq
    z = place[1] * bz - 5 + 4 * (row % nq) + lane // c1
    inside = (y >= 0) & (y < total_y) & (z >= 0) & (z < total_z)
    fine_mask[...] = jnp.where(inside, 1.0, 0.0)
    shape = (ny_mid * nq, 2 * c2)
    row = lax.broadcasted_iota(jnp.int32, shape, 0)
    lane = lax.broadcasted_iota(jnp.int32, shape, 1)
    y = place[0] * (by // 2) - 2 + row // nq
    z = place[1] * (bz // 2) - 2 + 2 * (row % nq) + lane // c2
    inside = (y >= 0) & (y < total_y // 2) & (z >= 0) & (z < total_z // 2)
    coarse_mask[...] = jnp.where(inside, 1.0, 0.0)

    emb[0] = jnp.zeros(emb.shape[1:], F32)
    emb[nx + 1] = jnp.zeros(emb.shape[1:], F32)
    fine[0, 0] = jnp.zeros(fine.shape[2:], F32)
    coarse[0] = jnp.zeros(coarse.shape[1:], F32)
    coarse[coarse_x + 1] = jnp.zeros(coarse.shape[1:], F32)
    grads[0] = jnp.zeros(grads.shape[1:], F32)
    grads[coarse_x + 1] = jnp.zeros(grads.shape[1:], F32)

    emb_rows = ny_emb * nq

    def embed(step, carry):
        start = pl.multiple_of(step * 2 * emb_rows, 16)
        values = feat[pl.ds(start, 2 * emb_rows), :]
        wide = values.astype(F32)
        grain = lax.broadcasted_iota(jnp.int32, (1, grains), 1).astype(F32) + 1.0
        picks = [
            jnp.where(wide[:, quad * k + quad - 1 : quad * k + quad] == grain, 1.0, 0.0).astype(BF16)
            for k in range(4)
        ]
        mixture = jnp.dot(values, wide_weight[...], preferred_element_type=F32) + jnp.dot(
            jnp.concatenate(picks, axis=1), wide_table[...], preferred_element_type=F32
        )
        out = silu(mixture).astype(BF16).astype(F32)
        emb[pl.ds(1 + 2 * step, 2), :, :, :lanes] = out.reshape(2, ny_emb, nq, lanes)
        following = next_row(out[:, :half])
        emb[pl.ds(1 + 2 * step, 2), :, :, lanes:] = following.reshape(2, ny_emb, nq, half)
        return carry

    lax.fori_loop(0, nx // 2, embed, 0)

    fine_step = 4

    def fine_conv(step, carry):
        x0 = step * fine_step
        patches = jnp.concatenate(
            [
                flat(emb[pl.ds(x0 + kx, fine_step), ky : ky + ny_fine]).astype(BF16)
                for kx, ky in TAPS_XY
            ],
            axis=1,
        )
        values = lax.dot_general(
            patches, band_fine[...], CONTRACT_LANES, preferred_element_type=F32
        )
        rows = ny_fine * nq
        for i in range(fine_step):
            layer = silu(values[i * rows : (i + 1) * rows]) * fine_mask[...]
            layer = layer.astype(BF16).astype(F32)
            following = next_row(layer[:, :half])
            for j in range(ny_fine):
                target = (x0 // 2 + (1 + i) // 2, (1 + i) % 2, j // 2, j % 2)
                fine[target + (slice(None), slice(0, lanes))] = layer[j * nq : (j + 1) * nq]
                fine[target + (slice(None), slice(lanes, None))] = following[j * nq : (j + 1) * nq]
        return carry

    lax.fori_loop(0, nx // fine_step, fine_conv, 0)

    mid_step = 4

    def down_conv(step, carry):
        x0 = step * mid_step
        taps = [
            flat(
                fine[pl.ds(x0 + kx // 2, mid_step), kx % 2, ky // 2 : ky // 2 + ny_mid, ky % 2]
            ).astype(BF16)
            for kx, ky in TAPS_XY
        ]
        parts = []
        for k in range(2):
            patches = jnp.concatenate(
                [tap[:, 2 * k * c1 : 2 * k * c1 + lanes] for tap in taps], axis=1
            )
            parts.append(
                lax.dot_general(
                    patches, band_down[...], CONTRACT_LANES, preferred_element_type=F32
                )
            )
        values = jnp.concatenate(parts, axis=1)
        pre[pl.ds(x0, mid_step)] = values.reshape(mid_step, ny_mid, nq, 2 * c2)
        inside = coarse_mask[...]
        inside = jnp.concatenate([inside] * mid_step, axis=0)
        act = (silu(values) * inside).astype(BF16).astype(F32)
        where = pl.ds(1 + x0, mid_step)
        whole = (mid_step, ny_mid, nq)
        coarse[where, :, :, :c2] = previous_row(act[:, c2:]).reshape(whole + (c2,))
        coarse[where, :, :, c2 : 3 * c2] = act.reshape(whole + (2 * c2,))
        coarse[where, :, :, 3 * c2 :] = next_row(act[:, :c2]).reshape(whole + (c2,))
        return carry

    lax.fori_loop(0, coarse_x // mid_step, down_conv, 0)

    bot_rows = ny_bot * nq

    def bottle_conv(step, carry):
        x0 = step * mid_step
        taps = [
            flat(coarse[pl.ds(x0 + kx, mid_step), ky : ky + ny_bot]).astype(BF16)
            for kx, ky in TAPS_XY
        ]
        parts = []
        for k in range(2):
            patches = jnp.concatenate([tap[:, k * c2 : (k + 3) * c2] for tap in taps], axis=1)
            parts.append(
                lax.dot_general(
                    patches, kernel_bottle[...], CONTRACT_LANES, preferred_element_type=F32
                )
            )
        values = jnp.concatenate(parts, axis=1)
        start = pl.multiple_of(x0 * bot_rows, 16)
        grad = cotangent[pl.ds(start, mid_step * bot_rows), :].astype(F32) * silu_grad(values)
        grad = grad.astype(BF16).astype(F32)
        where = pl.ds(1 + x0, mid_step)
        whole = (mid_step, ny_bot, nq)
        grads[where, :, :, :outs] = previous_row(grad[:, outs:]).reshape(whole + (outs,))
        grads[where, :, :, outs : 3 * outs] = grad.reshape(whole + (2 * outs,))
        grads[where, :, :, 3 * outs :] = next_row(grad[:, :outs]).reshape(whole + (outs,))
        act = silu(values).reshape(whole + (2 * outs,))[:, 1 : 1 + ny_own]
        start = pl.multiple_of(x0 * ny_own * nq, 16)
        bottle_out[pl.ds(start, mid_step * ny_own * nq), :] = flat(act).astype(BF16)
        return carry

    lax.fori_loop(0, coarse_x // mid_step, bottle_conv, 0)

    stacked = jnp.concatenate(
        [kernel_bottle[:, t * c2 : (t + 1) * c2] for t in range(27)], axis=0
    )
    own_rows = ny_own * nq

    def transpose_conv(step, carry):
        x0 = step * mid_step
        taps = [
            flat(grads[pl.ds(x0 + 2 - kx, mid_step), 2 - ky : 2 - ky + ny_own]).astype(BF16)
            for kx, ky in TAPS_XY
        ]
        parts = []
        for k in range(2):
            patches = jnp.concatenate(
                [
                    tap[:, (k + 2 - kz) * outs : (k + 3 - kz) * outs]
                    for tap in taps
                    for kz in range(3)
                ],
                axis=1,
            )
            parts.append(
                lax.dot_general(patches, stacked, CONTRACT_PLAIN, preferred_element_type=F32)
            )
        values = jnp.concatenate(parts, axis=1)
        start = pl.multiple_of(x0 * own_rows, 16)
        act_out[pl.ds(start, mid_step * own_rows), :] = values.astype(BF16)
        return carry

    lax.fori_loop(0, coarse_x // mid_step, transpose_conv, 0)

    scale = 1.0 / math.sqrt(coarse_x * (total_y // 2) * (total_z // 2))
    own = flat(grads[1 : 1 + coarse_x, 1 : 1 + ny_own, :, outs : 3 * outs])
    place_row = lax.broadcasted_iota(jnp.int32, own.shape, 0) % nq
    own = jnp.where((place_row >= 1) & (place_row <= bz // 4), own, 0.0)
    turned = jnp.transpose(own, (1, 0)).astype(BF16)
    for number, (kx, ky) in enumerate(TAPS_XY):
        rows = flat(coarse[kx : kx + coarse_x, ky + 1 : ky + 1 + ny_own]).astype(BF16)
        product = jnp.dot(turned, rows, preferred_element_type=F32)
        total = product[:outs, : 3 * c2] + product[outs:, c2:]
        total = jnp.transpose(total * scale, (1, 0)).astype(BF16)
        grad_out[number * 3 * c2 : (number + 1) * 3 * c2, :] = total

    first = place[2] * own_x
    fine_out[...] = fine[pl.ds(first, own_x + 1), :, 2 : 3 + ny_own]
    slope = silu_grad(pre[pl.ds(first, own_x), 2 : 2 + ny_own])
    slope_out[...] = flat(slope)


def down_kernel(mine, other, slope, fine, grad_out, *, dims):
    bz, c1, c2, nq, scale = dims
    own_x, ny_own = fine.shape[0] - 1, fine.shape[2] - 1
    grad = jnp.sum(other[...].astype(F32), axis=0) + mine[...].astype(F32)
    grad = (grad * slope[...]).astype(BF16).astype(F32)
    place_row = lax.broadcasted_iota(jnp.int32, grad.shape, 0) % nq
    grad = jnp.where((place_row >= 1) & (place_row <= bz // 4), grad, 0.0)
    turned = jnp.transpose(grad, (1, 0)).astype(BF16)
    for number, (kx, ky) in enumerate(TAPS_XY):
        rows = flat(
            fine[kx // 2 : kx // 2 + own_x, kx % 2, ky // 2 : ky // 2 + ny_own, ky % 2]
        ).astype(BF16)
        product = jnp.dot(turned, rows, preferred_element_type=F32)
        total = product[:c2, : 4 * c1] + product[c2:, 2 * c1 : 6 * c1]
        total = jnp.transpose(total * scale, (1, 0))[: 3 * c1].astype(BF16)
        grad_out[number * 3 * c1 : (number + 1) * 3 * c1, :] = total


def shifted(block, axis, step):
    count = lax.axis_size(axis)
    pairs = [(i, i + step) for i in range(count) if 0 <= i + step < count]
    return lax.ppermute(block, axis, pairs)


def with_halo(block, axis, dim, low, high):
    size = block.shape[dim]
    before = shifted(lax.slice_in_dim(block, size - low, size, axis=dim), axis, 1)
    after = shifted(lax.slice_in_dim(block, 0, high, axis=dim), axis, -1)
    return jnp.concatenate([before, block, after], axis=dim)


def scatter_sum(block, axis, distance):
    count = lax.axis_size(axis)
    index = lax.axis_index(axis)
    rest = block.shape[1:]
    bit = 1
    while bit < count:
        split = block.reshape((-1, 2) + rest)
        mine = (index // bit) % 2
        keep = lax.dynamic_index_in_dim(split, mine, 1, keepdims=False)
        send = lax.dynamic_index_in_dim(split, 1 - mine, 1, keepdims=False)
        got = lax.ppermute(send, axis, [(i, i ^ bit) for i in range(count)])
        block = (keep.astype(F32) + got.astype(F32)).astype(BF16)
        bit *= 2
    return block[0]


def per_device(
    fields, grain_ids, material_table, input_weight, kernel_fine, kernel_down, kernel_bottle,
    cotangent,
):
    comps, bx, by, bz = fields.shape
    grains, c1 = material_table.shape
    c2 = kernel_down.shape[0]
    outs_true = kernel_bottle.shape[0]
    gx, gy, gz = lax.axis_size("gx"), lax.axis_size("gy"), lax.axis_size("gz")
    nx, total_y, total_z = bx * gx, by * gy, bz * gz
    coarse_x = nx // 2
    nq = -(-(bz + 12) // 32) * 8
    outs = -(-outs_true // 128) * 128
    if outs != outs_true:
        kernel_bottle = jnp.pad(kernel_bottle, ((0, outs - outs_true), (0, 0)))
        cotangent = jnp.pad(cotangent, ((0, outs - outs_true), (0, 0), (0, 0), (0, 0)))

    quad = comps + 1
    feat = jnp.concatenate([fields, (grain_ids + 1).astype(BF16)[None]], axis=0)
    feat = jnp.transpose(feat, (1, 2, 3, 0)).reshape(bx, by, bz * quad)
    feat = lax.all_gather(feat, "gx", axis=0, tiled=True)
    feat = with_halo(feat, "gy", 1, 6, 5)
    feat = with_halo(feat, "gz", 2, 6 * quad, 6 * quad)
    feat = feat.reshape(nx, by + 11, (bz + 12) // 4, 4 * quad)
    feat = jnp.pad(feat, ((0, 0), (0, 0), (0, nq - feat.shape[2]), (0, 0)))
    feat = feat.reshape(-1, 4 * quad)

    cot = jnp.transpose(cotangent, (1, 2, 3, 0))
    cot = with_halo(cot, "gy", 1, 1, 1)
    cot = with_halo(cot, "gz", 2, 1, 1)
    cot = jnp.pad(cot, ((0, 0), (0, 0), (1, 2 * nq - bz // 2 - 3), (0, 0)))
    cot = cot.reshape(-1, 2 * outs)

    eye = jnp.eye(4, dtype=BF16)
    tall = jnp.pad(input_weight.T, ((0, 1), (0, 0)))
    wide_weight = jnp.kron(eye, tall)
    wide_table = jnp.kron(eye, material_table)
    split = kernel_fine.reshape(c1, 9, 3 * c1)
    band_fine = jnp.concatenate(
        [jnp.pad(split, ((0, 0), (0, 0), (k * c1, (3 - k) * c1))) for k in range(4)], axis=0
    ).reshape(4 * c1, 9 * 6 * c1)
    band_down = jnp.pad(kernel_down.reshape(c2, 9, 3 * c1), ((0, 0), (0, 0), (0, c1)))
    band_down = band_down.reshape(c2, 9 * 4 * c1)
    place = jnp.stack([lax.axis_index("gy"), lax.axis_index("gz"), lax.axis_index("gx")])

    ny_own, ny_mid, ny_bot = by // 2, by // 2 + 4, by // 2 + 2
    own_x = bx // 2
    lanes = 6 * c1
    vmem = pl.BlockSpec(memory_space=pltpu.VMEM)
    bottle_rows, act, bottle_part, fine_own, slope = pl.pallas_call(
        lambda *refs: forward_kernel(
            *refs, dims=(nx, by, bz, c1, c2, outs, grains, (total_y, total_z))
        ),
        out_shape=(
            jax.ShapeDtypeStruct((coarse_x * ny_own * nq, 2 * outs), BF16),
            jax.ShapeDtypeStruct((coarse_x * ny_own * nq, 2 * c2), BF16),
            jax.ShapeDtypeStruct((27 * c2, outs), BF16),
            jax.ShapeDtypeStruct((own_x + 1, 2, ny_own + 1, 2, nq, lanes), F32),
            jax.ShapeDtypeStruct((own_x * ny_own * nq, 2 * c2), F32),
        ),
        in_specs=[pl.BlockSpec(memory_space=pltpu.SMEM)] + [vmem] * 7,
        out_specs=(vmem,) * 5,
        scratch_shapes=[
            pltpu.VMEM((nx + 2, by + 11, nq, lanes), F32),
            pltpu.VMEM((coarse_x + 1, 2, (by + 10) // 2, 2, nq, lanes), F32),
            pltpu.VMEM((coarse_x + 2, ny_mid, nq, 4 * c2), F32),
            pltpu.VMEM((coarse_x + 2, ny_bot, nq, 4 * outs), F32),
            pltpu.VMEM((coarse_x, ny_mid, nq, 2 * c2), F32),
            pltpu.VMEM(((by + 9) * nq, 4 * c1), F32),
            pltpu.VMEM((ny_mid * nq, 2 * c2), F32),
        ],
        compiler_params=pltpu.CompilerParams(vmem_limit_bytes=60 * 1024 * 1024),
        name="forward",
    )(place, feat, wide_weight, wide_table, band_fine, band_down, kernel_bottle, cot)

    bottle = bottle_rows.reshape(coarse_x, ny_own, 2 * nq, outs)[:, :, 2 : 2 + bz // 2]
    bottle = jnp.transpose(bottle, (3, 0, 1, 2))[:outs_true]

    act = act.reshape(gx, own_x * ny_own * nq, 2 * c2)
    index = lax.axis_index("gx")
    mine = lax.dynamic_index_in_dim(act, index, 0, keepdims=False)
    if gx == 2:
        other = lax.dynamic_index_in_dim(act, 1 - index, 0, keepdims=True)
        other = lax.ppermute(other, "gx", [(0, 1), (1, 0)])
    else:
        spread = lax.all_to_all(act, "gx", 0, 0, tiled=True)
        others = [(index + k) % gx for k in range(1, gx)]
        other = jnp.concatenate([lax.dynamic_slice_in_dim(spread, k, 1, 0) for k in others], axis=0)

    scale = 1.0 / math.sqrt(coarse_x * (total_y // 2) * (total_z // 2))
    down_part = pl.pallas_call(
        lambda *refs: down_kernel(*refs, dims=(bz, c1, c2, nq, scale)),
        out_shape=jax.ShapeDtypeStruct((27 * c1, c2), BF16),
        in_specs=[vmem] * 4,
        out_specs=vmem,
        name="down_gradient",
    )(mine, other, slope, fine_own)

    def reduce_chunks(part):
        rows, width = part.shape
        part = part.reshape(gy, gz, rows // (gy * gz), width)
        part = jnp.transpose(part, (1, 0, 2, 3))
        part = scatter_sum(part, "gz", 1)
        return scatter_sum(part, "gy", 1)

    grad_bottle = reduce_chunks(bottle_part)[:, :outs_true].astype(F32).T
    down_part = down_part.reshape(27 * c1, gx, c2 // gx)
    down_part = scatter_sum(jnp.transpose(down_part, (1, 0, 2)), "gx", 1)
    grad_down = reduce_chunks(down_part).astype(F32).T
    return (bottle, grad_down, grad_bottle)


def solution(mesh):
    placed = (
        P(None, "gx", "gy", "gz"),
        P("gx", "gy", "gz"),
        P(),
        P(),
        P(),
        P(),
        P("gx", None),
        P("gx", None, "gy", "gz"),
    )
    return jax.shard_map(
        per_device,
        mesh=mesh,
        in_specs=placed,
        out_specs=(P("gx", None, "gy", "gz"), P("gx", ("gy", "gz")), P("gx", ("gy", "gz"))),
        check_vma=False,
    )
```

```python
import math

import jax
import jax.numpy as jnp
from jax import lax
from jax.experimental import pallas as pl
from jax.experimental.pallas import tpu as pltpu
from jax.sharding import PartitionSpec as P

F32 = jnp.float32
BF16 = jnp.bfloat16
CONTRACT_LANES = (((1,), (1,)), ((), ()))
CONTRACT_PLAIN = (((1,), (0,)), ((), ()))
TAPS_XY = [(kx, ky) for kx in range(3) for ky in range(3)]


def silu(values):
    return values / (1.0 + jnp.exp(-values))


def silu_grad(values):
    sigmoid = 1.0 / (1.0 + jnp.exp(-values))
    return sigmoid * (1.0 + values * (1.0 - sigmoid))


def flat(values):
    return values.reshape(-1, values.shape[-1])


def next_row(values):
    return pltpu.roll(values, values.shape[0] - 1, 0)


def previous_row(values):
    return pltpu.roll(values, 1, 0)


def shift_rows(values, forward):
    rows = flat(values)
    return (next_row(rows) if forward else previous_row(rows)).reshape(values.shape)


def forward_kernel(
    place, feat, wide_weight, wide_table, band_fine, band_down, kernel_bottle, cotangent,
    bottle_out, mine_out, others_out, grad_out, fine_out, slope_out,
    emb, fine, coarse, grads, pre, fine_mask, coarse_mask, *, dims,
):
    nx, by, bz, c1, c2, outs, grains, limits = dims
    total_y, total_z = limits
    ny_emb, ny_fine, ny_mid, ny_bot, ny_own = by + 11, by + 9, by // 2 + 4, by // 2 + 2, by // 2
    quad = feat.shape[1] // 4
    nq = emb.shape[2]
    coarse_x = nx // 2
    own_x = slope_out.shape[0] // (ny_own * nq)
    groups = coarse_x // own_x
    lanes = 4 * c1
    half = lanes // 2

    shape = (ny_fine * nq, lanes)
    row = lax.broadcasted_iota(jnp.int32, shape, 0)
    lane = lax.broadcasted_iota(jnp.int32, shape, 1)
    y = place[0] * by - 5 + row // nq
    z = place[1] * bz - 5 + 4 * (row % nq) + lane // c1
    inside = (y >= 0) & (y < total_y) & (z >= 0) & (z < total_z)
    fine_mask[...] = jnp.where(inside, 1.0, 0.0)
    shape = (ny_mid * nq, 2 * c2)
    row = lax.broadcasted_iota(jnp.int32, shape, 0)
    lane = lax.broadcasted_iota(jnp.int32, shape, 1)
    y = place[0] * (by // 2) - 2 + row // nq
    z = place[1] * (bz // 2) - 2 + 2 * (row % nq) + lane // c2
    inside = (y >= 0) & (y < total_y // 2) & (z >= 0) & (z < total_z // 2)
    coarse_mask[...] = jnp.where(inside, 1.0, 0.0)

    emb[0] = jnp.zeros(emb.shape[1:], F32)
    emb[nx + 1] = jnp.zeros(emb.shape[1:], F32)
    fine[0, 0] = jnp.zeros(fine.shape[2:], F32)
    coarse[0] = jnp.zeros(coarse.shape[1:], F32)
    coarse[coarse_x + 1] = jnp.zeros(coarse.shape[1:], F32)
    grads[0] = jnp.zeros(grads.shape[1:], F32)
    grads[coarse_x + 1] = jnp.zeros(grads.shape[1:], F32)

    emb_rows = ny_emb * nq

    def embed(step, carry):
        start = pl.multiple_of(step * 2 * emb_rows, 16)
        values = feat[pl.ds(start, 2 * emb_rows), :]
        wide = values.astype(F32)
        grain = lax.broadcasted_iota(jnp.int32, (1, grains), 1).astype(F32) + 1.0
        picks = [
            jnp.where(wide[:, quad * k + quad - 1 : quad * k + quad] == grain, 1.0, 0.0).astype(BF16)
            for k in range(4)
        ]
        mixture = lax.dot_general(
            values, wide_weight[...], CONTRACT_LANES, preferred_element_type=F32
        ) + jnp.dot(
            jnp.concatenate(picks, axis=1), wide_table[...], preferred_element_type=F32
        )
        out = silu(mixture).astype(BF16).astype(F32)
        emb[pl.ds(1 + 2 * step, 2), :, :, :lanes] = out.reshape(2, ny_emb, nq, lanes)
        following = next_row(out[:, :half])
        emb[pl.ds(1 + 2 * step, 2), :, :, lanes:] = following.reshape(2, ny_emb, nq, half)
        return carry

    lax.fori_loop(0, nx // 2, embed, 0)

    fine_step = 4

    def fine_conv(step, carry):
        x0 = step * fine_step
        patches = jnp.concatenate(
            [
                flat(emb[pl.ds(x0 + kx, fine_step), ky : ky + ny_fine]).astype(BF16)
                for kx, ky in TAPS_XY
            ],
            axis=1,
        )
        values = lax.dot_general(
            patches, band_fine[...], CONTRACT_LANES, preferred_element_type=F32
        )
        rows = ny_fine * nq
        for i in range(fine_step):
            layer = silu(values[i * rows : (i + 1) * rows]) * fine_mask[...]
            layer = layer.astype(BF16).astype(F32)
            following = next_row(layer[:, :half])
            for j in range(ny_fine):
                target = (x0 // 2 + (1 + i) // 2, (1 + i) % 2, j // 2, j % 2)
                fine[target + (slice(None), slice(0, lanes))] = layer[j * nq : (j + 1) * nq]
                fine[target + (slice(None), slice(lanes, None))] = following[j * nq : (j + 1) * nq]
        return carry

    lax.fori_loop(0, nx // fine_step, fine_conv, 0)

    mid_step = 4

    def down_conv(step, carry):
        x0 = step * mid_step
        taps = [
            flat(
                fine[pl.ds(x0 + kx // 2, mid_step), kx % 2, ky // 2 : ky // 2 + ny_mid, ky % 2]
            ).astype(BF16)
            for kx, ky in TAPS_XY
        ]
        parts = []
        for k in range(2):
            patches = jnp.concatenate(
                [tap[:, 2 * k * c1 : 2 * k * c1 + lanes] for tap in taps], axis=1
            )
            parts.append(
                lax.dot_general(
                    patches, band_down[...], CONTRACT_LANES, preferred_element_type=F32
                )
            )
        values = jnp.concatenate(parts, axis=1)
        pre[pl.ds(x0, mid_step)] = values.reshape(mid_step, ny_mid, nq, 2 * c2)
        inside = coarse_mask[...]
        inside = jnp.concatenate([inside] * mid_step, axis=0)
        act = (silu(values) * inside).astype(BF16).astype(F32)
        where = pl.ds(1 + x0, mid_step)
        whole = (mid_step, ny_mid, nq)
        coarse[where, :, :, :c2] = previous_row(act[:, c2:]).reshape(whole + (c2,))
        coarse[where, :, :, c2 : 3 * c2] = act.reshape(whole + (2 * c2,))
        coarse[where, :, :, 3 * c2 :] = next_row(act[:, :c2]).reshape(whole + (c2,))
        return carry

    lax.fori_loop(0, coarse_x // mid_step, down_conv, 0)

    bot_rows = ny_bot * nq

    def bottle_conv(step, carry):
        x0 = step * mid_step
        taps = [
            flat(coarse[pl.ds(x0 + kx, mid_step), ky : ky + ny_bot]).astype(BF16)
            for kx, ky in TAPS_XY
        ]
        parts = []
        for k in range(2):
            patches = jnp.concatenate([tap[:, k * c2 : (k + 3) * c2] for tap in taps], axis=1)
            parts.append(
                lax.dot_general(
                    patches, kernel_bottle[...], CONTRACT_LANES, preferred_element_type=F32
                )
            )
        values = jnp.concatenate(parts, axis=1)
        start = pl.multiple_of(x0 * bot_rows, 16)
        grad = cotangent[pl.ds(start, mid_step * bot_rows), :].astype(F32) * silu_grad(values)
        grad = grad.astype(BF16).astype(F32)
        where = pl.ds(1 + x0, mid_step)
        whole = (mid_step, ny_bot, nq)
        grads[where, :, :, :outs] = previous_row(grad[:, outs:]).reshape(whole + (outs,))
        grads[where, :, :, outs : 3 * outs] = grad.reshape(whole + (2 * outs,))
        grads[where, :, :, 3 * outs :] = next_row(grad[:, :outs]).reshape(whole + (outs,))
        act = silu(values).reshape(whole + (2 * outs,))[:, 1 : 1 + ny_own]
        start = pl.multiple_of(x0 * ny_own * nq, 16)
        bottle_out[pl.ds(start, mid_step * ny_own * nq), :] = flat(act).astype(BF16)
        return carry

    lax.fori_loop(0, coarse_x // mid_step, bottle_conv, 0)

    stacked = jnp.concatenate(
        [kernel_bottle[:, t * c2 : (t + 1) * c2] for t in range(27)], axis=0
    )
    own_rows = ny_own * nq

    def transpose_conv(step, carry):
        x0 = step * mid_step
        taps = [
            flat(grads[pl.ds(x0 + 2 - kx, mid_step), 2 - ky : 2 - ky + ny_own]).astype(BF16)
            for kx, ky in TAPS_XY
        ]
        parts = []
        for k in range(2):
            patches = jnp.concatenate(
                [
                    tap[:, (k + 2 - kz) * outs : (k + 3 - kz) * outs]
                    for tap in taps
                    for kz in range(3)
                ],
                axis=1,
            )
            parts.append(
                lax.dot_general(patches, stacked, CONTRACT_PLAIN, preferred_element_type=F32)
            )
        values = jnp.concatenate(parts, axis=1)
        values = values.astype(BF16)
        owner = lax.rem(x0 // own_x - place[2] + groups, groups)
        inner = lax.rem(x0, own_x)

        @pl.when(owner == 0)
        def _():
            start = pl.multiple_of(inner * own_rows, 16)
            mine_out[pl.ds(start, mid_step * own_rows), :] = values

        @pl.when(owner > 0)
        def _():
            start = pl.multiple_of(inner * own_rows, 16)
            others_out[owner - 1, pl.ds(start, mid_step * own_rows), :] = values

        return carry

    lax.fori_loop(0, coarse_x // mid_step, transpose_conv, 0)

    scale = 1.0 / math.sqrt(coarse_x * (total_y // 2) * (total_z // 2))
    own = flat(grads[1 : 1 + coarse_x, 1 : 1 + ny_own, :, outs : 3 * outs])
    place_row = lax.broadcasted_iota(jnp.int32, own.shape, 0) % nq
    own = jnp.where((place_row >= 1) & (place_row <= bz // 4), own, 0.0)
    turned = jnp.transpose(own, (1, 0)).astype(BF16)
    for number, (kx, ky) in enumerate(TAPS_XY):
        rows = flat(coarse[kx : kx + coarse_x, ky + 1 : ky + 1 + ny_own]).astype(BF16)
        product = jnp.dot(turned, rows, preferred_element_type=F32)
        total = product[:outs, : 3 * c2] + product[outs:, c2:]
        total = jnp.transpose(total * scale, (1, 0)).astype(BF16)
        grad_out[number * 3 * c2 : (number + 1) * 3 * c2, :] = total

    first = place[2] * own_x
    fine_out[...] = fine[pl.ds(first, own_x + 1), :, 2 : 3 + ny_own]
    slope = silu_grad(pre[pl.ds(first, own_x), 2 : 2 + ny_own])
    slope_out[...] = flat(slope)


def prepare_kernel(
    input_weight, table, kernel_fine, kernel_down, weight_out, table_out, fine_out, down_out
):
    c1, comps = input_weight.shape
    grains = table.shape[0]
    c2 = kernel_down.shape[0]
    quad = comps + 1
    weight_out[...] = jnp.zeros(weight_out.shape, BF16)
    table_out[...] = jnp.zeros(table_out.shape, BF16)
    weight = input_weight[...]
    for k in range(4):
        weight_out[k * c1 : (k + 1) * c1, k * quad : k * quad + comps] = weight
        table_out[k * grains : (k + 1) * grains, k * c1 : (k + 1) * c1] = table[...]
    width = 3 * c1
    for tap in range(9):
        piece = kernel_fine[:, tap * width : (tap + 1) * width].astype(F32)
        for k in range(4):
            parts = [piece]
            if k:
                parts.insert(0, jnp.zeros((c1, k * c1), F32))
            if k < 3:
                parts.append(jnp.zeros((c1, (3 - k) * c1), F32))
            fine_out[k * c1 : (k + 1) * c1, tap * 2 * width : (tap + 1) * 2 * width] = (
                jnp.concatenate(parts, axis=1).astype(BF16)
            )
        piece = kernel_down[:, tap * width : (tap + 1) * width].astype(F32)
        piece = jnp.concatenate([piece, jnp.zeros((c2, c1), F32)], axis=1)
        down_out[:, tap * 4 * c1 : (tap + 1) * 4 * c1] = piece.astype(BF16)


def down_kernel(mine, other, slope, fine, grad_out, total_ref, *, dims):
    bz, c1, c2, nq, scale = dims
    own_x, ny_own = fine.shape[0] - 1, fine.shape[2] - 1
    grad = jnp.sum(other[...].astype(F32), axis=0) + mine[...].astype(F32)
    grad = (grad * slope[...]).astype(BF16).astype(F32)
    place_row = lax.broadcasted_iota(jnp.int32, grad.shape, 0) % nq
    grad = jnp.where((place_row >= 1) & (place_row <= bz // 4), grad, 0.0)
    turned = jnp.transpose(grad, (1, 0)).astype(BF16)
    for number, (kx, ky) in enumerate(TAPS_XY):
        rows = flat(
            fine[kx // 2 : kx // 2 + own_x, kx % 2, ky // 2 : ky // 2 + ny_own, ky % 2]
        ).astype(BF16)
        product = jnp.dot(turned, rows, preferred_element_type=F32)
        total = product[:c2, : 4 * c1] + product[c2:, 2 * c1 : 6 * c1]
        total = jnp.transpose(total * scale, (1, 0))[: 3 * c1]
        total_ref[number * 3 * c1 : (number + 1) * 3 * c1, :] = total
    if len(grad_out.shape) == 2:
        grad_out[...] = total_ref[...].astype(BF16)
        return
    chunks, rows = grad_out.shape[1:3]
    low = lax.broadcasted_iota(jnp.int32, (rows, c2), 1) < c2 // 2
    for k in range(chunks):
        first = total_ref[2 * k * rows : (2 * k + 1) * rows, :]
        second = total_ref[(2 * k + 1) * rows : (2 * k + 2) * rows, :]
        grad_out[0, k] = jnp.where(low, first, pltpu.roll(second, c2 // 2, 1)).astype(BF16)
        grad_out[1, k] = jnp.where(low, pltpu.roll(first, c2 // 2, 1), second).astype(BF16)


def ring_halo(forward, backward, axis):
    count = lax.axis_size(axis)
    index = lax.axis_index(axis)
    before = lax.ppermute(forward, axis, [(i, (i + 1) % count) for i in range(count)])
    after = lax.ppermute(backward, axis, [(i, (i - 1) % count) for i in range(count)])
    zero = jnp.zeros((), before.dtype)
    return jnp.where(index > 0, before, zero), jnp.where(index < count - 1, after, zero)


def halve(block, axes, bit):
    count = math.prod(lax.axis_size(axis) for axis in axes)
    index = lax.axis_index(axes)
    split = block.reshape((-1, 2) + block.shape[1:])
    mine = (index // bit) % 2
    keep = lax.dynamic_index_in_dim(split, mine, 1, keepdims=False)
    send = lax.dynamic_index_in_dim(split, 1 - mine, 1, keepdims=False)
    got = lax.ppermute(send, axes, [(i, i ^ bit) for i in range(count)])
    return keep.astype(F32) + got.astype(F32)


def halve_all(block, axes, bit=1):
    while block.shape[0] > 1:
        block = halve(block.astype(BF16), axes, bit)
        bit *= 2
    return block[0]


def per_device(
    fields, grain_ids, material_table, input_weight, kernel_fine, kernel_down, kernel_bottle,
    cotangent,
):
    comps, bx, by, bz = fields.shape
    grains, c1 = material_table.shape
    c2 = kernel_down.shape[0]
    outs_true = kernel_bottle.shape[0]
    gx, gy, gz = lax.axis_size("gx"), lax.axis_size("gy"), lax.axis_size("gz")
    nx, total_y, total_z = bx * gx, by * gy, bz * gz
    coarse_x = nx // 2
    nq = -(-(bz + 12) // 32) * 8
    outs = -(-outs_true // 128) * 128
    if outs != outs_true:
        kernel_bottle = jnp.pad(kernel_bottle, ((0, outs - outs_true), (0, 0)))
        cotangent = jnp.pad(cotangent, ((0, outs - outs_true), (0, 0), (0, 0), (0, 0)))

    quad = comps + 1
    half_y, half_z = by // 2, bz // 2
    feat = jnp.concatenate([fields, (grain_ids + 1).astype(BF16)[None]], axis=0)
    feat = jnp.transpose(feat, (1, 2, 3, 0)).reshape(bx, by, bz * quad)
    feat = lax.all_gather(feat, "gx", axis=0, tiled=True)
    cot = jnp.transpose(cotangent, (1, 2, 3, 0))

    def packed(first, second):
        return jnp.concatenate([first.reshape(-1, 128), second.reshape(-1, 128)], axis=0)

    def unpacked(both, first_shape, second_shape):
        cut = math.prod(first_shape) // 128
        return both[:cut].reshape(first_shape), both[cut:].reshape(second_shape)

    before, after = ring_halo(
        packed(feat[:, by - 6 :], cot[:, half_y - 1 :]), packed(feat[:, :5], cot[:, :1]), "gy"
    )
    edge = (coarse_x, 1, half_z, outs)
    feat_before, cot_before = unpacked(before, (nx, 6, bz * quad), edge)
    feat_after, cot_after = unpacked(after, (nx, 5, bz * quad), edge)
    feat = jnp.concatenate([feat_before, feat, feat_after], axis=1)
    cot = jnp.concatenate([cot_before, cot, cot_after], axis=1)
    before, after = ring_halo(packed(feat, cot[:, :, half_z - 1 :]), packed(feat, cot[:, :, :1]), "gz")
    edge = (coarse_x, half_y + 2, 1, outs)
    feat_before, cot_before = unpacked(before, feat.shape, edge)
    feat_after, cot_after = unpacked(after, feat.shape, edge)
    feat = jnp.concatenate(
        [feat_before[:, :, (bz - 6) * quad :], feat, feat_after[:, :, : 6 * quad]], axis=2
    )
    feat = jnp.pad(feat, ((0, 0), (0, 0), (0, 4 * nq * quad - feat.shape[2])))
    feat = feat.reshape(-1, 4 * quad)
    gap = (coarse_x, half_y + 2, 2 * nq - half_z - 3, outs)
    cot = jnp.concatenate(
        [jnp.zeros(edge, BF16), cot_before, cot, cot_after, jnp.zeros(gap, BF16)], axis=2
    )
    cot = cot.reshape(-1, 2 * outs)

    vmem = pl.BlockSpec(memory_space=pltpu.VMEM)
    wide_weight, wide_table, band_fine, band_down = pl.pallas_call(
        prepare_kernel,
        out_shape=(
            jax.ShapeDtypeStruct((4 * c1, 4 * quad), BF16),
            jax.ShapeDtypeStruct((4 * grains, 4 * c1), BF16),
            jax.ShapeDtypeStruct((4 * c1, 9 * 6 * c1), BF16),
            jax.ShapeDtypeStruct((c2, 9 * 4 * c1), BF16),
        ),
        in_specs=[vmem] * 4,
        out_specs=(vmem,) * 4,
        cost_estimate=pl.CostEstimate(flops=10**9, transcendentals=0, bytes_accessed=4 * 10**6),
        name="prepare",
    )(input_weight, material_table, kernel_fine, kernel_down)
    place = jnp.stack([lax.axis_index("gy"), lax.axis_index("gz"), lax.axis_index("gx")])

    ny_own, ny_mid, ny_bot = by // 2, by // 2 + 4, by // 2 + 2
    own_x = bx // 2
    lanes = 6 * c1
    own_rows = own_x * ny_own * nq
    bottle_rows, mine, others, bottle_part, fine_own, slope = pl.pallas_call(
        lambda *refs: forward_kernel(
            *refs, dims=(nx, by, bz, c1, c2, outs, grains, (total_y, total_z))
        ),
        out_shape=(
            jax.ShapeDtypeStruct((coarse_x * ny_own * nq, 2 * outs), BF16),
            jax.ShapeDtypeStruct((own_rows, 2 * c2), BF16),
            jax.ShapeDtypeStruct((gx - 1, own_rows, 2 * c2), BF16),
            jax.ShapeDtypeStruct((27 * c2, outs), BF16),
            jax.ShapeDtypeStruct((own_x + 1, 2, ny_own + 1, 2, nq, lanes), F32),
            jax.ShapeDtypeStruct((own_x * ny_own * nq, 2 * c2), F32),
        ),
        in_specs=[pl.BlockSpec(memory_space=pltpu.SMEM)] + [vmem] * 7,
        out_specs=(vmem,) * 6,
        scratch_shapes=[
            pltpu.VMEM((nx + 2, by + 11, nq, lanes), F32),
            pltpu.VMEM((coarse_x + 1, 2, (by + 10) // 2, 2, nq, lanes), F32),
            pltpu.VMEM((coarse_x + 2, ny_mid, nq, 4 * c2), F32),
            pltpu.VMEM((coarse_x + 2, ny_bot, nq, 4 * outs), F32),
            pltpu.VMEM((coarse_x, ny_mid, nq, 2 * c2), F32),
            pltpu.VMEM(((by + 9) * nq, 4 * c1), F32),
            pltpu.VMEM((ny_mid * nq, 2 * c2), F32),
        ],
        compiler_params=pltpu.CompilerParams(vmem_limit_bytes=60 * 1024 * 1024),
        cost_estimate=pl.CostEstimate(flops=10**10, transcendentals=0, bytes_accessed=10**7),
        name="forward",
    )(place, feat, wide_weight, wide_table, band_fine, band_down, kernel_bottle, cot)

    bottle = bottle_rows.reshape(coarse_x, ny_own, 2 * nq, outs)[:, :, 2 : 2 + bz // 2]
    bottle = jnp.transpose(bottle, (3, 0, 1, 2))[:outs_true]

    other = jnp.stack(
        [
            lax.ppermute(others[k - 1], "gx", [(i, (i + k) % gx) for i in range(gx)])
            for k in range(1, gx)
        ]
    )

    chunks = gy * gz
    rows = 27 * c1 // chunks
    side_by_side = gx == 2 and rows % 2 == 0
    part_shape = (2, chunks, rows // 2, c2) if side_by_side else (27 * c1, c2)
    scale = 1.0 / math.sqrt(coarse_x * (total_y // 2) * (total_z // 2))
    down_part = pl.pallas_call(
        lambda *refs: down_kernel(*refs, dims=(bz, c1, c2, nq, scale)),
        out_shape=jax.ShapeDtypeStruct(part_shape, BF16),
        in_specs=[vmem] * 4,
        out_specs=vmem,
        scratch_shapes=[pltpu.VMEM((27 * c1, c2), F32)],
        cost_estimate=pl.CostEstimate(flops=2 * 10**9, transcendentals=0, bytes_accessed=10**6),
        name="down_gradient",
    )(mine, other, slope, fine_own)

    both = ("gy", "gz")
    bottle_part = bottle_part.reshape(chunks, 27 * c2 // chunks, outs)
    if side_by_side:
        bottle_part = halve(bottle_part, both, 1).astype(BF16)
        bottle_part = halve(bottle_part, both, 2).astype(BF16)
        turned = jnp.moveaxis(down_part, 0, 1)
        turned = halve(turned, both, 1).astype(BF16)
        down_part = halve(jnp.moveaxis(turned, 1, 0), ("gx",), 1).astype(BF16)[0]
        down_part = halve(down_part, both, 2).astype(BF16)
        summed = halve_all(jnp.concatenate([bottle_part, down_part], axis=1), both, 4)
        cut = bottle_part.shape[1]
        grad_bottle = summed[:cut, :outs_true].T
        halves = summed[cut:]
        grad_down = jnp.concatenate([halves[:, : c2 // 2].T, halves[:, c2 // 2 :].T], axis=1)
    else:
        grad_bottle = halve_all(bottle_part, both)[:, :outs_true].T
        down_part = jnp.transpose(down_part.reshape(27 * c1, gx, c2 // gx), (1, 0, 2))
        down_part = halve_all(down_part, ("gx",)).reshape(chunks, rows, c2 // gx)
        grad_down = halve_all(down_part, both).T
    return (bottle, grad_down, grad_bottle)


def solution(mesh):
    placed = (
        P(None, "gx", "gy", "gz"),
        P("gx", "gy", "gz"),
        P(),
        P(),
        P(),
        P(),
        P("gx", None),
        P("gx", None, "gy", "gz"),
    )
    return jax.shard_map(
        per_device,
        mesh=mesh,
        in_specs=placed,
        out_specs=(P("gx", None, "gy", "gz"), P("gx", ("gy", "gz")), P("gx", ("gy", "gz"))),
        check_vma=False,
    )
```

```python
import math

import jax
import jax.numpy as jnp
from jax import lax
from jax.experimental import pallas as pl
from jax.experimental.pallas import tpu as pltpu
from jax.sharding import PartitionSpec as P

F32 = jnp.float32
BF16 = jnp.bfloat16
CONTRACT_LANES = (((1,), (1,)), ((), ()))
CONTRACT_PLAIN = (((1,), (0,)), ((), ()))
LANES = 128
FINE_STEP = 8
MID_STEP = 4
TAPS_XY = [(kx, ky) for kx in range(3) for ky in range(3)]


def silu(values):
    half = 0.5 * values
    return half + half * jnp.tanh(half)


def silu_grad(values):
    sigmoid = 0.5 + 0.5 * jnp.tanh(0.5 * values)
    return sigmoid * (1.0 + values * (1.0 - sigmoid))


def flat(values):
    return values.reshape(-1, values.shape[-1])


def next_row(values):
    return pltpu.roll(values, values.shape[0] - 1, 0)


def previous_row(values):
    return pltpu.roll(values, 1, 0)


def pack_kernel(fields, grain_ids, out):
    comps, bx, by, bz = fields.shape
    quad = comps + 1
    column = lax.broadcasted_iota(jnp.int32, (bz, bz * quad), 1)
    row = lax.broadcasted_iota(jnp.int32, (bz, bz * quad), 0)
    total = jnp.zeros((bx * by, bz * quad), F32)
    for c in range(quad):
        plane = fields[c].astype(F32) if c < comps else (grain_ids[...] + 1).astype(F32)
        spread = jnp.where(column == row * quad + c, 1.0, 0.0).astype(BF16)
        total = total + jnp.dot(flat(plane).astype(BF16), spread, preferred_element_type=F32)
    out[...] = total.astype(BF16)


def widen_inputs(weight, table, weight_out, table_out):
    comps, c1 = weight.shape
    grains = table.shape[1]
    quad = comps + 1
    weight_out[...] = jnp.zeros(weight_out.shape, F32)
    table_out[...] = jnp.zeros(table_out.shape, BF16)
    entries = jnp.transpose(table[...].astype(F32), (1, 0)).astype(BF16)
    for k in range(4):
        weight_out[k * quad : k * quad + comps, k * c1 : (k + 1) * c1] = weight[...].astype(F32)
        table_out[k * grains : (k + 1) * grains, k * c1 : (k + 1) * c1] = entries


def widen_kernels(kernel_fine, kernel_down, fine_out, down_out):
    c1 = kernel_fine.shape[0]
    width = 3 * c1
    turned = jnp.transpose(kernel_fine[...].astype(F32), (1, 0))
    fine_out[...] = jnp.zeros(fine_out.shape, BF16)
    for tap in range(9):
        piece = turned[tap * width : (tap + 1) * width].astype(BF16)
        for k in range(4):
            start = tap * 2 * width + k * c1
            fine_out[start : start + width, k * c1 : (k + 1) * c1] = piece
        start = tap * 4 * c1
        down_out[start : start + width, :] = kernel_down[tap * width : (tap + 1) * width, :]
        down_out[start + width : start + 4 * c1, :] = jnp.zeros((c1, down_out.shape[1]), BF16)


def forward_kernel(
    place, feat, near, far, cot, weight, table, kernel_fine, kernel_down, kernel_bottle,
    bottle_out, mine_out, others_out, grad_out, slope_out, kept_out,
    emb, fine, coarse, grads, pre, fine_mask, coarse_mask, wide_feat, cot_rows, cotangent,
    wide_weight, wide_table, band_fine, band_down, *, dims,
):
    nx, by, bz, c1, c2, outs, grains, limits = dims
    total_y, total_z = limits
    ny_emb, ny_fine, ny_mid, ny_bot, ny_own = by + 11, by + 9, by // 2 + 4, by // 2 + 2, by // 2
    quad = weight.shape[0] + 1
    nq = fine.shape[4]
    coarse_x = nx // 2
    own_x = slope_out.shape[0] // (ny_own * nq)
    groups = coarse_x // own_x
    lanes = 4 * c1
    half = lanes // 2
    half_z = bz // 2

    widen_inputs(weight, table, wide_weight, wide_table)

    emb_rows = nx * ny_emb
    has_before = place[1] > 0
    has_after = place[1] < total_z // bz - 1
    odd = place[1] % 2 == 1
    near_all, far_all = near[...].astype(F32), far[...].astype(F32)
    before = jnp.where(has_before, jnp.where(odd, near_all, far_all), 0.0)
    after = jnp.where(has_after, jnp.where(odd, far_all, near_all), 0.0)
    low, high = before[:emb_rows], after[:emb_rows]
    spare = jnp.zeros((emb_rows, 4 * nq * quad - (bz + 12) * quad), F32)
    wide_feat[...] = jnp.concatenate(
        [low[:, (bz - 6) * quad :], feat[...].astype(F32), high[:, : 6 * quad], spare], axis=1
    )
    columns = coarse_x * ny_bot
    cotangent[...] = jnp.zeros(cotangent.shape, F32)
    edge_low = before[emb_rows:].reshape(-1, outs)
    edge_high = after[emb_rows:].reshape(-1, outs)
    slabs = outs // LANES
    cot_wide = cot[...].astype(F32)
    for k in range(slabs):
        cot_rows[k] = cot_wide[:, k * LANES : (k + 1) * LANES]
        for z in range(half_z):
            target = (z % 2 * slabs + k, pl.ds(z // 2 + 1, columns, stride=nq))
            cotangent[target] = cot_rows[k, pl.ds(z, columns, stride=half_z)]
        cotangent[slabs + k, pl.ds(0, columns, stride=nq)] = edge_low[:, k * LANES : (k + 1) * LANES]
        cotangent[k, pl.ds(half_z // 2 + 1, columns, stride=nq)] = edge_high[:, k * LANES : (k + 1) * LANES]

    shape = (ny_fine * nq, lanes)
    row = lax.broadcasted_iota(jnp.int32, shape, 0)
    lane = lax.broadcasted_iota(jnp.int32, shape, 1)
    y = place[0] * by - 5 + row // nq
    z = place[1] * bz - 5 + 4 * (row % nq) + lane // c1
    inside = (y >= 0) & (y < total_y) & (z >= 0) & (z < total_z)
    fine_mask[...] = jnp.where(inside, 1.0, 0.0)
    shape = (ny_mid * nq, 2 * c2)
    row = lax.broadcasted_iota(jnp.int32, shape, 0)
    lane = lax.broadcasted_iota(jnp.int32, shape, 1)
    y = place[0] * (by // 2) - 2 + row // nq
    z = place[1] * (bz // 2) - 2 + 2 * (row % nq) + lane // c2
    inside = (y >= 0) & (y < total_y // 2) & (z >= 0) & (z < total_z // 2)
    coarse_mask[...] = jnp.where(inside, 1.0, 0.0)

    layer_rows = ny_emb * nq
    blank = jnp.zeros((emb.shape[0], layer_rows, LANES), F32)
    emb[:, :layer_rows] = blank
    emb[:, (nx + 1) * layer_rows :] = blank
    fine[0, 0] = jnp.zeros(fine.shape[2:], F32)
    coarse[0] = jnp.zeros(coarse.shape[1:], F32)
    coarse[coarse_x + 1] = jnp.zeros(coarse.shape[1:], F32)
    grads[0] = jnp.zeros(grads.shape[1:], F32)
    grads[coarse_x + 1] = jnp.zeros(grads.shape[1:], F32)

    emb_step = 8
    chunk = emb_step * ny_emb

    def embed(step, carry):
        start = pl.multiple_of(step * chunk, 8)
        values = wide_feat[pl.ds(start, chunk), :]
        grain = lax.broadcasted_iota(jnp.int32, (1, grains), 1).astype(F32) + 1.0
        base = start * nq + layer_rows
        for q in range(nq):
            part = values[:, 4 * quad * q : 4 * quad * (q + 1)]
            picks = [
                jnp.where(part[:, quad * k + quad - 1 : quad * k + quad] == grain, 1.0, 0.0)
                for k in range(4)
            ]
            picks = jnp.concatenate([pick.astype(BF16) for pick in picks], axis=1)
            mixture = jnp.dot(
                part.astype(BF16), wide_weight[...].astype(BF16), preferred_element_type=F32
            ) + jnp.dot(picks, wide_table[...], preferred_element_type=F32)
            out = silu(mixture).astype(BF16).astype(F32)
            following = out[:, :half] if q else jnp.zeros((chunk, half), F32)
            for k in range(lanes // LANES):
                target = (k, pl.ds(base + q, chunk, stride=nq))
                emb[target] = out[:, k * LANES : (k + 1) * LANES]
            for k in range(half // LANES):
                target = (lanes // LANES + k, pl.ds(base + (q - 1) % nq, chunk, stride=nq))
                emb[target] = following[:, k * LANES : (k + 1) * LANES]
        return carry

    lax.fori_loop(0, nx // emb_step, embed, 0)

    widen_kernels(kernel_fine, kernel_down, band_fine, band_down)

    fine_step = FINE_STEP

    def fine_conv(step, carry):
        x0 = step * fine_step

        def layers(kx, ky):
            pieces = []
            for i in range(fine_step):
                start = pl.multiple_of((x0 + i + kx) * layer_rows + ky * nq, 8)
                pieces.append(
                    jnp.concatenate(
                        [emb[k, pl.ds(start, ny_fine * nq)] for k in range(emb.shape[0])], axis=1
                    )
                )
            return jnp.concatenate(pieces, axis=0).astype(BF16)

        patches = jnp.concatenate([layers(kx, ky) for kx, ky in TAPS_XY], axis=1)
        values = lax.dot_general(
            patches, band_fine[...], CONTRACT_PLAIN, preferred_element_type=F32
        )
        rows = ny_fine * nq
        for i in range(fine_step):
            layer = silu(values[i * rows : (i + 1) * rows]) * fine_mask[...]
            layer = layer.astype(BF16).astype(F32)
            following = next_row(layer[:, :half])
            for j in range(ny_fine):
                target = (x0 // 2 + (1 + i) // 2, (1 + i) % 2, j // 2, j % 2)
                fine[target + (slice(None), slice(0, lanes))] = layer[j * nq : (j + 1) * nq]
                fine[target + (slice(None), slice(lanes, None))] = following[j * nq : (j + 1) * nq]
        return carry

    lax.fori_loop(0, nx // fine_step, fine_conv, 0)

    first = place[2] * own_x
    kept_out[...] = flat(fine[pl.ds(first, own_x + 1), :, 2 : 3 + ny_own]).astype(BF16)

    mid_step = MID_STEP if coarse_x % MID_STEP == 0 else own_x

    def down_conv(step, carry):
        x0 = step * mid_step
        taps = [
            flat(
                fine[pl.ds(x0 + kx // 2, mid_step), kx % 2, ky // 2 : ky // 2 + ny_mid, ky % 2]
            ).astype(BF16)
            for kx, ky in TAPS_XY
        ]
        patches = jnp.concatenate(
            [
                jnp.concatenate([tap[:, 2 * k * c1 : 2 * k * c1 + lanes] for tap in taps], axis=1)
                for k in range(2)
            ],
            axis=0,
        )
        values = side_by_side(
            lax.dot_general(patches, band_down[...], CONTRACT_PLAIN, preferred_element_type=F32)
        )
        pre[pl.ds(x0, mid_step)] = values.reshape(mid_step, ny_mid, nq, 2 * c2)
        inside = coarse_mask[...]
        inside = jnp.concatenate([inside] * mid_step, axis=0)
        act = (silu(values) * inside).astype(BF16).astype(F32)
        where = pl.ds(1 + x0, mid_step)
        whole = (mid_step, ny_mid, nq)
        coarse[where, :, :, :c2] = previous_row(act[:, c2:]).reshape(whole + (c2,))
        coarse[where, :, :, c2 : 3 * c2] = act.reshape(whole + (2 * c2,))
        coarse[where, :, :, 3 * c2 :] = next_row(act[:, :c2]).reshape(whole + (c2,))
        return carry

    lax.fori_loop(0, coarse_x // mid_step, down_conv, 0)

    bot_rows = ny_bot * nq

    def bottle_conv(step, carry):
        x0 = step * mid_step
        taps = [
            flat(coarse[pl.ds(x0 + kx, mid_step), ky : ky + ny_bot]).astype(BF16)
            for kx, ky in TAPS_XY
        ]
        patches = jnp.concatenate(
            [
                jnp.concatenate([tap[:, k * c2 : (k + 3) * c2] for tap in taps], axis=1)
                for k in range(2)
            ],
            axis=0,
        )
        values = side_by_side(
            lax.dot_general(
                patches, kernel_bottle[...], CONTRACT_LANES, preferred_element_type=F32
            )
        )
        start = pl.multiple_of(x0 * bot_rows, 8)
        spread = [
            cotangent[k, pl.ds(start, mid_step * bot_rows)] for k in range(cotangent.shape[0])
        ]
        grad = jnp.concatenate(spread, axis=1) * silu_grad(values)
        grad = grad.astype(BF16).astype(F32)
        where = pl.ds(1 + x0, mid_step)
        whole = (mid_step, ny_bot, nq)
        grads[where, :, :, :outs] = previous_row(grad[:, outs:]).reshape(whole + (outs,))
        grads[where, :, :, outs : 3 * outs] = grad.reshape(whole + (2 * outs,))
        grads[where, :, :, 3 * outs :] = next_row(grad[:, :outs]).reshape(whole + (outs,))
        act = silu(values).reshape(whole + (2 * outs,))[:, 1 : 1 + ny_own]
        start = pl.multiple_of(x0 * ny_own * nq, 16)
        bottle_out[pl.ds(start, mid_step * ny_own * nq), :] = flat(act).astype(BF16)
        return carry

    lax.fori_loop(0, coarse_x // mid_step, bottle_conv, 0)

    stacked = jnp.concatenate(
        [kernel_bottle[:, t * c2 : (t + 1) * c2] for t in range(27)], axis=0
    )
    own_rows = ny_own * nq

    def transpose_conv(step, carry):
        x0 = step * mid_step
        taps = [
            flat(grads[pl.ds(x0 + 2 - kx, mid_step), 2 - ky : 2 - ky + ny_own]).astype(BF16)
            for kx, ky in TAPS_XY
        ]
        patches = jnp.concatenate(
            [
                jnp.concatenate(
                    [
                        tap[:, (k + 2 - kz) * outs : (k + 3 - kz) * outs]
                        for tap in taps
                        for kz in range(3)
                    ],
                    axis=1,
                )
                for k in range(2)
            ],
            axis=0,
        )
        values = side_by_side(
            lax.dot_general(patches, stacked, CONTRACT_PLAIN, preferred_element_type=F32)
        )
        values = values.astype(BF16)
        for k in range(mid_step // own_x):
            piece = values[k * own_x * own_rows : (k + 1) * own_x * own_rows]
            owner = lax.rem(x0 // own_x + k - place[2] + groups, groups)

            @pl.when(owner == 0)
            def _(piece=piece):
                mine_out[...] = piece

            @pl.when(owner > 0)
            def _(piece=piece, owner=owner):
                others_out[owner - 1] = piece

        return carry

    lax.fori_loop(0, coarse_x // mid_step, transpose_conv, 0)

    scale = 1.0 / math.sqrt(coarse_x * (total_y // 2) * (total_z // 2))
    own = flat(grads[1 : 1 + coarse_x, 1 : 1 + ny_own, :, outs : 3 * outs])
    place_row = lax.broadcasted_iota(jnp.int32, own.shape, 0) % nq
    own = jnp.where((place_row >= 1) & (place_row <= bz // 4), own, 0.0)
    turned = jnp.transpose(own, (1, 0)).astype(BF16)
    for number, (kx, ky) in enumerate(TAPS_XY):
        rows = flat(coarse[kx : kx + coarse_x, ky + 1 : ky + 1 + ny_own]).astype(BF16)
        product = jnp.dot(turned, rows, preferred_element_type=F32)
        total = product[:outs, : 3 * c2] + product[outs:, c2:]
        total = jnp.transpose(total * scale, (1, 0)).astype(BF16)
        grad_out[number * 3 * c2 : (number + 1) * 3 * c2, :] = total

    slope = silu_grad(pre[pl.ds(first, own_x), 2 : 2 + ny_own])
    slope_out[...] = flat(slope)


def down_kernel(mine, other, slope, kept, grad_out, total_ref, fine, *, dims):
    bz, c1, c2, nq, scale = dims
    own_x, ny_own = fine.shape[0] - 1, fine.shape[2] - 1
    grad = jnp.sum(other[...].astype(F32), axis=0) + mine[...].astype(F32)
    grad = (grad * slope[...]).astype(BF16).astype(F32)
    place_row = lax.broadcasted_iota(jnp.int32, grad.shape, 0) % nq
    grad = jnp.where((place_row >= 1) & (place_row <= bz // 4), grad, 0.0)
    turned = jnp.transpose(grad, (1, 0)).astype(BF16)
    fine[...] = kept[...].astype(F32).reshape(fine.shape)
    for number, (kx, ky) in enumerate(TAPS_XY):
        rows = flat(
            fine[kx // 2 : kx // 2 + own_x, kx % 2, ky // 2 : ky // 2 + ny_own, ky % 2]
        ).astype(BF16)
        product = jnp.dot(turned, rows, preferred_element_type=F32)
        total = product[:c2, : 4 * c1] + product[c2:, 2 * c1 : 6 * c1]
        total = jnp.transpose(total * scale, (1, 0))[: 3 * c1]
        total_ref[number * 3 * c1 : (number + 1) * 3 * c1, :] = total
    if len(grad_out.shape) == 2:
        grad_out[...] = total_ref[...].astype(BF16)
        return
    chunks, rows = grad_out.shape[0], grad_out.shape[2]
    low = lax.broadcasted_iota(jnp.int32, (rows, c2), 1) < c2 // 2
    for k in range(chunks):
        first = total_ref[2 * k * rows : (2 * k + 1) * rows, :]
        second = total_ref[(2 * k + 1) * rows : (2 * k + 2) * rows, :]
        grad_out[k, 0] = jnp.where(low, first, pltpu.roll(second, c2 // 2, 1)).astype(BF16)
        grad_out[k, 1] = jnp.where(low, pltpu.roll(first, c2 // 2, 1), second).astype(BF16)


def halo(forward, backward, axis):
    count = lax.axis_size(axis)
    before = lax.ppermute(forward, axis, [(i, (i + 1) % count) for i in range(count)])
    after = lax.ppermute(backward, axis, [(i, (i - 1) % count) for i in range(count)])
    return before, after


def swap_halo(forward, backward, axis):
    count = lax.axis_size(axis)
    odd = lax.axis_index(axis) % 2 == 1
    if count % 2:
        before, after = halo(forward, backward, axis)
        return jnp.where(odd, before, after), jnp.where(odd, after, before)
    near = lax.ppermute(
        jnp.where(odd, backward, forward), axis, [(i, i ^ 1) for i in range(count)]
    )
    far = lax.ppermute(
        jnp.where(odd, forward, backward),
        axis,
        [(i, (i + (1 if i % 2 else -1)) % count) for i in range(count)],
    )
    return near, far


def open_halo(forward, backward, axis):
    count = lax.axis_size(axis)
    index = lax.axis_index(axis)
    before, after = halo(forward, backward, axis)
    zero = jnp.zeros((), before.dtype)
    return jnp.where(index > 0, before, zero), jnp.where(index < count - 1, after, zero)


def side_by_side(values):
    rows = values.shape[0] // 2
    return jnp.concatenate([values[:rows], values[rows:]], axis=1)


def halve(block, axes, bit, dim=0):
    count = math.prod(lax.axis_size(axis) for axis in axes)
    index = lax.axis_index(axes)
    pairs = block.shape[:dim] + ((-1, 2) if block.shape[dim] > 2 else (2,))
    split = block.reshape(pairs + block.shape[dim + 1 :])
    dim = len(pairs) - 1
    mine = (index // bit) % 2
    keep = lax.dynamic_index_in_dim(split, mine, dim, keepdims=False)
    send = lax.dynamic_index_in_dim(split, 1 - mine, dim, keepdims=False)
    got = lax.ppermute(send, axes, [(i, i ^ bit) for i in range(count)])
    return keep.astype(F32) + got.astype(F32)


def halve_all(block, axes, bit=1):
    count = block.shape[0]
    while count > 1:
        block = halve(block.astype(BF16), axes, bit)
        bit, count = 2 * bit, count // 2
    return block


def window(
    fields, grain_ids, material_table, input_weight, kernel_fine, kernel_down, kernel_bottle,
    cotangent,
):
    comps, bx, by, bz = fields.shape
    grains, c1 = material_table.shape
    c2 = kernel_down.shape[0]
    outs_true = kernel_bottle.shape[0]
    gx, gy, gz = lax.axis_size("gx"), lax.axis_size("gy"), lax.axis_size("gz")
    nx, total_y, total_z = bx * gx, by * gy, bz * gz
    coarse_x = nx // 2
    nq = -(-(bz + 12) // 32) * 8
    outs = -(-outs_true // 128) * 128
    if outs != outs_true:
        kernel_bottle = jnp.pad(kernel_bottle, ((0, outs - outs_true), (0, 0)))
        cotangent = jnp.pad(cotangent, ((0, outs - outs_true), (0, 0), (0, 0), (0, 0)))

    quad = comps + 1
    half_y, half_z = by // 2, bz // 2
    vmem = pl.BlockSpec(memory_space=pltpu.VMEM)
    feat = pl.pallas_call(
        pack_kernel,
        out_shape=jax.ShapeDtypeStruct((bx * by, bz * quad), BF16),
        in_specs=[vmem] * 2,
        out_specs=vmem,
        compiler_params=pltpu.CompilerParams(vmem_limit_bytes=4 << 20),
        name="pack",
    )(fields, grain_ids)
    feat = lax.all_gather(feat.reshape(bx, by, bz * quad), "gx", axis=0, tiled=True)
    cot = jnp.transpose(cotangent, (1, 2, 3, 0))

    def packed(first, second):
        return jnp.concatenate([first.reshape(-1, 128), second.reshape(-1, 128)], axis=0)

    def unpacked(both, first_shape, second_shape):
        cut = math.prod(first_shape) // 128
        return both[:cut].reshape(first_shape), both[cut:].reshape(second_shape)

    before, after = open_halo(
        packed(feat[:, by - 6 :], cot[:, half_y - 1 :]), packed(feat[:, :5], cot[:, :1]), "gy"
    )
    edge = (coarse_x, 1, half_z, outs)
    feat_before, cot_before = unpacked(before, (nx, 6, bz * quad), edge)
    feat_after, cot_after = unpacked(after, (nx, 5, bz * quad), edge)
    feat = jnp.concatenate([feat_before, feat, feat_after], axis=1)
    cot = jnp.concatenate([cot_before, cot, cot_after], axis=1)
    near, far = swap_halo(
        packed(feat, cot[:, :, half_z - 1 :]), packed(feat, cot[:, :, :1]), "gz"
    )
    place = jnp.stack([lax.axis_index("gy"), lax.axis_index("gz"), lax.axis_index("gx")])

    ny_own, ny_mid, ny_bot = by // 2, by // 2 + 4, by // 2 + 2
    own_x = bx // 2
    lanes = 6 * c1
    own_rows = own_x * ny_own * nq
    kept = (own_x + 1, 2, ny_own + 1, 2, nq, lanes)
    limit = min(60 << 20, (14 << 20) + nx * (5 << 17))
    bottle_rows, mine, others, bottle_part, slope, fine_own = pl.pallas_call(
        lambda *refs: forward_kernel(
            *refs, dims=(nx, by, bz, c1, c2, outs, grains, (total_y, total_z))
        ),
        out_shape=(
            jax.ShapeDtypeStruct((coarse_x * ny_own * nq, 2 * outs), BF16),
            jax.ShapeDtypeStruct((own_rows, 2 * c2), BF16),
            jax.ShapeDtypeStruct((gx - 1, own_rows, 2 * c2), BF16),
            jax.ShapeDtypeStruct((27 * c2, outs), BF16),
            jax.ShapeDtypeStruct((own_x * ny_own * nq, 2 * c2), F32),
            jax.ShapeDtypeStruct((math.prod(kept[:-1]), lanes), BF16),
        ),
        in_specs=[pl.BlockSpec(memory_space=pltpu.SMEM)] + [vmem] * 9,
        out_specs=(vmem,) * 6,
        scratch_shapes=[
            pltpu.VMEM((lanes // LANES, (nx + 2) * (by + 11) * nq, LANES), F32),
            pltpu.VMEM((coarse_x + 1, 2, (by + 10) // 2, 2, nq, lanes), F32),
            pltpu.VMEM((coarse_x + 2, ny_mid, nq, 4 * c2), F32),
            pltpu.VMEM((coarse_x + 2, ny_bot, nq, 4 * outs), F32),
            pltpu.VMEM((coarse_x, ny_mid, nq, 2 * c2), F32),
            pltpu.VMEM(((by + 9) * nq, 4 * c1), F32),
            pltpu.VMEM((ny_mid * nq, 2 * c2), F32),
            pltpu.VMEM((nx * (by + 11), 4 * nq * quad), F32),
            pltpu.VMEM((outs // LANES, coarse_x * ny_bot * bz // 2, LANES), F32),
            pltpu.VMEM((2 * outs // LANES, coarse_x * ny_bot * nq, LANES), F32),
            pltpu.VMEM((4 * quad, 4 * c1), F32),
            pltpu.VMEM((4 * grains, 4 * c1), BF16),
            pltpu.VMEM((9 * lanes, 4 * c1), BF16),
            pltpu.VMEM((9 * 4 * c1, c2), BF16),
        ],
        compiler_params=pltpu.CompilerParams(vmem_limit_bytes=limit),
        cost_estimate=pl.CostEstimate(flops=10**10, transcendentals=0, bytes_accessed=10**7),
        name="forward",
    )(
        place, feat.reshape(-1, bz * quad), near, far, cot.reshape(-1, outs),
        input_weight.T, material_table.T, kernel_fine, kernel_down.T, kernel_bottle,
    )

    bottle = bottle_rows.reshape(coarse_x, ny_own, 2 * nq, outs)[:, :, 2 : 2 + bz // 2]
    bottle = jnp.transpose(bottle, (3, 0, 1, 2))[:outs_true]

    other = jnp.stack(
        [
            lax.ppermute(others[k - 1], "gx", [(i, (i + k) % gx) for i in range(gx)])
            for k in range(1, gx)
        ]
    )

    chunks = gy * gz
    rows = 27 * c1 // chunks
    paired = gx == 2 and rows % 2 == 0
    part_shape = (chunks, 2, rows // 2, c2) if paired else (27 * c1, c2)
    scale = 1.0 / math.sqrt(coarse_x * (total_y // 2) * (total_z // 2))
    down_part = pl.pallas_call(
        lambda *refs: down_kernel(*refs, dims=(bz, c1, c2, nq, scale)),
        out_shape=jax.ShapeDtypeStruct(part_shape, BF16),
        in_specs=[vmem] * 4,
        out_specs=vmem,
        scratch_shapes=[
            pltpu.VMEM((27 * c1, c2), F32),
            pltpu.VMEM(kept, F32),
        ],
        compiler_params=pltpu.CompilerParams(vmem_limit_bytes=10 << 20),
        cost_estimate=pl.CostEstimate(flops=2 * 10**9, transcendentals=0, bytes_accessed=10**6),
        name="down_gradient",
    )(mine, other, slope, fine_own)

    both = ("gy", "gz")
    bottle_part = bottle_part.reshape(chunks, 27 * c2 // chunks, outs)
    if paired:
        bottle_part = halve(bottle_part, both, 1).astype(BF16)
        bottle_part = halve(bottle_part, both, 2).astype(BF16)
        down_part = halve(down_part, both, 1).astype(BF16)
        down_part = halve(down_part, ("gx",), 1, 1).astype(BF16)
        down_part = halve(down_part, both, 2).astype(BF16)
        summed = halve_all(jnp.concatenate([bottle_part, down_part], axis=1), both, 4)
        cut = bottle_part.shape[1]
        grad_bottle = summed[:cut, :outs_true].T
        halves = summed[cut:]
        grad_down = jnp.concatenate([halves[:, : c2 // 2].T, halves[:, c2 // 2 :].T], axis=1)
    else:
        grad_bottle = halve_all(bottle_part, both)[:, :outs_true].T
        down_part = jnp.transpose(down_part.reshape(27 * c1, gx, c2 // gx), (1, 0, 2))
        down_part = halve_all(down_part, ("gx",)).reshape(chunks, rows, c2 // gx)
        grad_down = halve_all(down_part, both).T
    return (bottle, grad_down, grad_bottle)


def solution(mesh):
    placed = (
        P(None, "gx", "gy", "gz"),
        P("gx", "gy", "gz"),
        P(),
        P(),
        P(),
        P(),
        P("gx", None),
        P("gx", None, "gy", "gz"),
    )
    return jax.shard_map(
        window,
        mesh=mesh,
        in_specs=placed,
        out_specs=(P("gx", None, "gy", "gz"), P("gx", ("gy", "gz")), P("gx", ("gy", "gz"))),
        check_vma=False,
    )
```

```python
import math

import jax
import jax.numpy as jnp
from jax import lax
from jax.experimental import pallas as pl
from jax.experimental.pallas import tpu as pltpu
from jax.sharding import PartitionSpec as P

F32 = jnp.float32
BF16 = jnp.bfloat16
CONTRACT_LANES = (((1,), (1,)), ((), ()))
CONTRACT_PLAIN = (((1,), (0,)), ((), ()))
LANES = 128
FINE_STEP = 8
MID_STEP = 4
TAPS_XY = [(kx, ky) for kx in range(3) for ky in range(3)]


def silu(values):
    half = 0.5 * values
    return half + half * jnp.tanh(half)


def silu_grad(values):
    sigmoid = 0.5 + 0.5 * jnp.tanh(0.5 * values)
    return sigmoid * (1.0 + values * (1.0 - sigmoid))


def flat(values):
    return values.reshape(-1, values.shape[-1])


def next_row(values):
    return pltpu.roll(values, values.shape[0] - 1, 0)


def previous_row(values):
    return pltpu.roll(values, 1, 0)


def pack_kernel(fields, grain_ids, cotangent, out, cot_out):
    comps, bx, by, bz = fields.shape
    quad = comps + 1
    column = lax.broadcasted_iota(jnp.int32, (bz, bz * quad), 1)
    row = lax.broadcasted_iota(jnp.int32, (bz, bz * quad), 0)
    total = jnp.zeros((bx * by, bz * quad), F32)
    for c in range(quad):
        plane = fields[c].astype(F32) if c < comps else (grain_ids[...] + 1).astype(F32)
        spread = jnp.where(column == row * quad + c, 1.0, 0.0).astype(BF16)
        total = total + jnp.dot(flat(plane).astype(BF16), spread, preferred_element_type=F32)
    out[...] = total.astype(BF16)
    cot_out[...] = cotangent[...]


def widen_inputs(weight, table, weight_out, table_out):
    comps, c1 = weight.shape
    grains = table.shape[1]
    quad = comps + 1
    weight_out[...] = jnp.zeros(weight_out.shape, F32)
    table_out[...] = jnp.zeros(table_out.shape, BF16)
    entries = jnp.transpose(table[...].astype(F32), (1, 0)).astype(BF16)
    for k in range(4):
        weight_out[k * quad : k * quad + comps, k * c1 : (k + 1) * c1] = weight[...].astype(F32)
        table_out[k * grains : (k + 1) * grains, k * c1 : (k + 1) * c1] = entries


def widen_kernels(kernel_fine, kernel_down, fine_out, down_out):
    c1 = kernel_fine.shape[0]
    width = 3 * c1
    turned = jnp.transpose(kernel_fine[...].astype(F32), (1, 0))
    fine_out[...] = jnp.zeros(fine_out.shape, BF16)
    for tap in range(9):
        piece = turned[tap * width : (tap + 1) * width].astype(BF16)
        for k in range(4):
            start = tap * 2 * width + k * c1
            fine_out[start : start + width, k * c1 : (k + 1) * c1] = piece
        start = tap * 4 * c1
        down_out[start : start + width, :] = kernel_down[tap * width : (tap + 1) * width, :]
        down_out[start + width : start + 4 * c1, :] = jnp.zeros((c1, down_out.shape[1]), BF16)


def forward_kernel(
    place, feat, near, far, cot, wide_weight, wide_table, kernel_fine, kernel_down, kernel_bottle,
    bottle_out, mine_out, others_out, grad_out, slope_out, kept_out,
    emb, fine, coarse, grads, pre, fine_mask, coarse_mask, wide_feat, cot_rows, cotangent,
    band_fine, band_down, *, dims,
):
    nx, by, bz, c1, c2, outs, grains, limits = dims
    total_y, total_z = limits
    ny_emb, ny_fine, ny_mid, ny_bot, ny_own = by + 11, by + 9, by // 2 + 4, by // 2 + 2, by // 2
    quad = wide_weight.shape[0] // 4
    nq = fine.shape[4]
    coarse_x = nx // 2
    own_x = slope_out.shape[0] // (ny_own * nq)
    groups = coarse_x // own_x
    lanes = 4 * c1
    half = lanes // 2
    half_z = bz // 2


    emb_rows = nx * ny_emb
    has_before = place[1] > 0
    has_after = place[1] < total_z // bz - 1
    odd = place[1] % 2 == 1
    near_all, far_all = near[...].astype(F32), far[...].astype(F32)
    before = jnp.where(has_before, jnp.where(odd, near_all, far_all), 0.0)
    after = jnp.where(has_after, jnp.where(odd, far_all, near_all), 0.0)
    low, high = before[:emb_rows], after[:emb_rows]
    spare = jnp.zeros((emb_rows, 4 * nq * quad - (bz + 12) * quad), F32)
    wide_feat[...] = jnp.concatenate(
        [low[:, (bz - 6) * quad :], feat[...].astype(F32), high[:, : 6 * quad], spare], axis=1
    )
    columns = coarse_x * ny_bot
    cotangent[...] = jnp.zeros(cotangent.shape, F32)
    edge_low = before[emb_rows:].reshape(-1, outs)
    edge_high = after[emb_rows:].reshape(-1, outs)
    slabs = outs // LANES
    cot_wide = cot[...].astype(F32)
    for k in range(slabs):
        cot_rows[k] = cot_wide[:, k * LANES : (k + 1) * LANES]
        for z in range(half_z):
            target = (z % 2 * slabs + k, pl.ds(z // 2 + 1, columns, stride=nq))
            cotangent[target] = cot_rows[k, pl.ds(z, columns, stride=half_z)]
        cotangent[slabs + k, pl.ds(0, columns, stride=nq)] = edge_low[:, k * LANES : (k + 1) * LANES]
        cotangent[k, pl.ds(half_z // 2 + 1, columns, stride=nq)] = edge_high[:, k * LANES : (k + 1) * LANES]

    shape = (ny_fine * nq, lanes)
    row = lax.broadcasted_iota(jnp.int32, shape, 0)
    lane = lax.broadcasted_iota(jnp.int32, shape, 1)
    y = place[0] * by - 5 + row // nq
    z = place[1] * bz - 5 + 4 * (row % nq) + lane // c1
    inside = (y >= 0) & (y < total_y) & (z >= 0) & (z < total_z)
    fine_mask[...] = jnp.where(inside, 1.0, 0.0)
    shape = (ny_mid * nq, 2 * c2)
    row = lax.broadcasted_iota(jnp.int32, shape, 0)
    lane = lax.broadcasted_iota(jnp.int32, shape, 1)
    y = place[0] * (by // 2) - 2 + row // nq
    z = place[1] * (bz // 2) - 2 + 2 * (row % nq) + lane // c2
    inside = (y >= 0) & (y < total_y // 2) & (z >= 0) & (z < total_z // 2)
    coarse_mask[...] = jnp.where(inside, 1.0, 0.0)

    layer_rows = ny_emb * nq
    blank = jnp.zeros((emb.shape[0], layer_rows, LANES), F32)
    emb[:, :layer_rows] = blank
    emb[:, (nx + 1) * layer_rows :] = blank
    fine[0, 0] = jnp.zeros(fine.shape[2:], F32)
    coarse[0] = jnp.zeros(coarse.shape[1:], F32)
    coarse[coarse_x + 1] = jnp.zeros(coarse.shape[1:], F32)
    grads[0] = jnp.zeros(grads.shape[1:], F32)
    grads[coarse_x + 1] = jnp.zeros(grads.shape[1:], F32)

    emb_step = 8
    chunk = emb_step * ny_emb

    def embed(step, carry):
        start = pl.multiple_of(step * chunk, 8)
        values = wide_feat[pl.ds(start, chunk), :]
        grain = lax.broadcasted_iota(jnp.int32, (1, grains), 1).astype(F32) + 1.0
        base = start * nq + layer_rows
        for q in range(nq):
            part = values[:, 4 * quad * q : 4 * quad * (q + 1)]
            picks = [
                jnp.where(part[:, quad * k + quad - 1 : quad * k + quad] == grain, 1.0, 0.0)
                for k in range(4)
            ]
            picks = jnp.concatenate([pick.astype(BF16) for pick in picks], axis=1)
            mixture = jnp.dot(
                part.astype(BF16), wide_weight[...].astype(BF16), preferred_element_type=F32
            ) + jnp.dot(picks, wide_table[...], preferred_element_type=F32)
            out = silu(mixture).astype(BF16).astype(F32)
            following = out[:, :half] if q else jnp.zeros((chunk, half), F32)
            for k in range(lanes // LANES):
                target = (k, pl.ds(base + q, chunk, stride=nq))
                emb[target] = out[:, k * LANES : (k + 1) * LANES]
            for k in range(half // LANES):
                target = (lanes // LANES + k, pl.ds(base + (q - 1) % nq, chunk, stride=nq))
                emb[target] = following[:, k * LANES : (k + 1) * LANES]
        return carry

    lax.fori_loop(0, nx // emb_step, embed, 0)

    widen_kernels(kernel_fine, kernel_down, band_fine, band_down)

    fine_step = FINE_STEP

    def fine_conv(step, carry):
        x0 = step * fine_step

        def layers(kx, ky):
            pieces = []
            for i in range(fine_step):
                start = pl.multiple_of((x0 + i + kx) * layer_rows + ky * nq, 8)
                pieces.append(
                    jnp.concatenate(
                        [emb[k, pl.ds(start, ny_fine * nq)] for k in range(emb.shape[0])], axis=1
                    )
                )
            return jnp.concatenate(pieces, axis=0).astype(BF16)

        patches = jnp.concatenate([layers(kx, ky) for kx, ky in TAPS_XY], axis=1)
        values = lax.dot_general(
            patches, band_fine[...], CONTRACT_PLAIN, preferred_element_type=F32
        )
        rows = ny_fine * nq
        for i in range(fine_step):
            layer = silu(values[i * rows : (i + 1) * rows]) * fine_mask[...]
            layer = layer.astype(BF16).astype(F32)
            following = next_row(layer[:, :half])
            for j in range(ny_fine):
                target = (x0 // 2 + (1 + i) // 2, (1 + i) % 2, j // 2, j % 2)
                fine[target + (slice(None), slice(0, lanes))] = layer[j * nq : (j + 1) * nq]
                fine[target + (slice(None), slice(lanes, None))] = following[j * nq : (j + 1) * nq]
        return carry

    lax.fori_loop(0, nx // fine_step, fine_conv, 0)

    first = place[2] * own_x
    kept_out[...] = flat(fine[pl.ds(first, own_x + 1), :, 2 : 3 + ny_own]).astype(BF16)

    mid_step = MID_STEP if coarse_x % MID_STEP == 0 else own_x

    def down_conv(step, carry):
        x0 = step * mid_step
        taps = [
            flat(
                fine[pl.ds(x0 + kx // 2, mid_step), kx % 2, ky // 2 : ky // 2 + ny_mid, ky % 2]
            ).astype(BF16)
            for kx, ky in TAPS_XY
        ]
        patches = jnp.concatenate(
            [
                jnp.concatenate([tap[:, 2 * k * c1 : 2 * k * c1 + lanes] for tap in taps], axis=1)
                for k in range(2)
            ],
            axis=0,
        )
        values = side_by_side(
            lax.dot_general(patches, band_down[...], CONTRACT_PLAIN, preferred_element_type=F32)
        )
        pre[pl.ds(x0, mid_step)] = values.reshape(mid_step, ny_mid, nq, 2 * c2)
        inside = coarse_mask[...]
        inside = jnp.concatenate([inside] * mid_step, axis=0)
        act = (silu(values) * inside).astype(BF16).astype(F32)
        where = pl.ds(1 + x0, mid_step)
        whole = (mid_step, ny_mid, nq)
        coarse[where, :, :, :c2] = previous_row(act[:, c2:]).reshape(whole + (c2,))
        coarse[where, :, :, c2 : 3 * c2] = act.reshape(whole + (2 * c2,))
        coarse[where, :, :, 3 * c2 :] = next_row(act[:, :c2]).reshape(whole + (c2,))
        return carry

    lax.fori_loop(0, coarse_x // mid_step, down_conv, 0)

    bot_rows = ny_bot * nq

    def bottle_conv(step, carry):
        x0 = step * mid_step
        taps = [
            flat(coarse[pl.ds(x0 + kx, mid_step), ky : ky + ny_bot]).astype(BF16)
            for kx, ky in TAPS_XY
        ]
        patches = jnp.concatenate(
            [
                jnp.concatenate([tap[:, k * c2 : (k + 3) * c2] for tap in taps], axis=1)
                for k in range(2)
            ],
            axis=0,
        )
        values = side_by_side(
            lax.dot_general(
                patches, kernel_bottle[...], CONTRACT_LANES, preferred_element_type=F32
            )
        )
        start = pl.multiple_of(x0 * bot_rows, 8)
        spread = [
            cotangent[k, pl.ds(start, mid_step * bot_rows)] for k in range(cotangent.shape[0])
        ]
        grad = jnp.concatenate(spread, axis=1) * silu_grad(values)
        grad = grad.astype(BF16).astype(F32)
        where = pl.ds(1 + x0, mid_step)
        whole = (mid_step, ny_bot, nq)
        grads[where, :, :, :outs] = previous_row(grad[:, outs:]).reshape(whole + (outs,))
        grads[where, :, :, outs : 3 * outs] = grad.reshape(whole + (2 * outs,))
        grads[where, :, :, 3 * outs :] = next_row(grad[:, :outs]).reshape(whole + (outs,))
        act = silu(values).reshape(whole + (2 * outs,))[:, 1 : 1 + ny_own]
        start = pl.multiple_of(x0 * ny_own * nq, 16)
        bottle_out[pl.ds(start, mid_step * ny_own * nq), :] = flat(act).astype(BF16)
        return carry

    lax.fori_loop(0, coarse_x // mid_step, bottle_conv, 0)

    stacked = jnp.concatenate(
        [kernel_bottle[:, t * c2 : (t + 1) * c2] for t in range(27)], axis=0
    )
    own_rows = ny_own * nq

    def transpose_conv(step, carry):
        x0 = step * mid_step
        taps = [
            flat(grads[pl.ds(x0 + 2 - kx, mid_step), 2 - ky : 2 - ky + ny_own]).astype(BF16)
            for kx, ky in TAPS_XY
        ]
        patches = jnp.concatenate(
            [
                jnp.concatenate(
                    [
                        tap[:, (k + 2 - kz) * outs : (k + 3 - kz) * outs]
                        for tap in taps
                        for kz in range(3)
                    ],
                    axis=1,
                )
                for k in range(2)
            ],
            axis=0,
        )
        values = side_by_side(
            lax.dot_general(patches, stacked, CONTRACT_PLAIN, preferred_element_type=F32)
        )
        values = values.astype(BF16)
        for k in range(mid_step // own_x):
            piece = values[k * own_x * own_rows : (k + 1) * own_x * own_rows]
            owner = lax.rem(x0 // own_x + k - place[2] + groups, groups)

            @pl.when(owner == 0)
            def _(piece=piece):
                mine_out[...] = piece

            @pl.when(owner > 0)
            def _(piece=piece, owner=owner):
                others_out[owner - 1] = piece

        return carry

    lax.fori_loop(0, coarse_x // mid_step, transpose_conv, 0)

    scale = 1.0 / math.sqrt(coarse_x * (total_y // 2) * (total_z // 2))
    own = flat(grads[1 : 1 + coarse_x, 1 : 1 + ny_own, :, outs : 3 * outs])
    place_row = lax.broadcasted_iota(jnp.int32, own.shape, 0) % nq
    own = jnp.where((place_row >= 1) & (place_row <= bz // 4), own, 0.0)
    turned = jnp.transpose(own, (1, 0)).astype(BF16)
    for number, (kx, ky) in enumerate(TAPS_XY):
        rows = flat(coarse[kx : kx + coarse_x, ky + 1 : ky + 1 + ny_own]).astype(BF16)
        product = jnp.dot(turned, rows, preferred_element_type=F32)
        total = product[:outs, : 3 * c2] + product[outs:, c2:]
        total = jnp.transpose(total * scale, (1, 0)).astype(BF16)
        grad_out[number * 3 * c2 : (number + 1) * 3 * c2, :] = total

    slope = silu_grad(pre[pl.ds(first, own_x), 2 : 2 + ny_own])
    slope_out[...] = flat(slope)


def down_kernel(mine, other, slope, kept, grad_out, total_ref, fine, *, dims):
    bz, c1, c2, nq, scale = dims
    own_x, ny_own = fine.shape[0] - 1, fine.shape[2] - 1
    grad = jnp.sum(other[...].astype(F32), axis=0) + mine[...].astype(F32)
    grad = (grad * slope[...]).astype(BF16).astype(F32)
    place_row = lax.broadcasted_iota(jnp.int32, grad.shape, 0) % nq
    grad = jnp.where((place_row >= 1) & (place_row <= bz // 4), grad, 0.0)
    turned = jnp.transpose(grad, (1, 0)).astype(BF16)
    fine[...] = kept[...].astype(F32).reshape(fine.shape)
    for number, (kx, ky) in enumerate(TAPS_XY):
        rows = flat(
            fine[kx // 2 : kx // 2 + own_x, kx % 2, ky // 2 : ky // 2 + ny_own, ky % 2]
        ).astype(BF16)
        product = jnp.dot(turned, rows, preferred_element_type=F32)
        total = product[:c2, : 4 * c1] + product[c2:, 2 * c1 : 6 * c1]
        total = jnp.transpose(total * scale, (1, 0))[: 3 * c1]
        total_ref[number * 3 * c1 : (number + 1) * 3 * c1, :] = total
    if len(grad_out.shape) == 2:
        grad_out[...] = total_ref[...].astype(BF16)
        return
    chunks, rows = grad_out.shape[0], grad_out.shape[2]
    low = lax.broadcasted_iota(jnp.int32, (rows, c2), 1) < c2 // 2
    for k in range(chunks):
        first = total_ref[2 * k * rows : (2 * k + 1) * rows, :]
        second = total_ref[(2 * k + 1) * rows : (2 * k + 2) * rows, :]
        grad_out[k, 0] = jnp.where(low, first, pltpu.roll(second, c2 // 2, 1)).astype(BF16)
        grad_out[k, 1] = jnp.where(low, pltpu.roll(first, c2 // 2, 1), second).astype(BF16)


def finish_kernel(index, joined, got, bottle_out, down_out):
    cut = bottle_out.shape[0]
    width = down_out.shape[0]
    total = joined[index[0]].astype(F32) + got[...].astype(F32)
    bottle_out[...] = total[:cut]
    turned = jnp.transpose(total[cut:], (1, 0))
    down_out[...] = jnp.concatenate([turned[:width], turned[width:]], axis=1)


def halo(forward, backward, axis):
    count = lax.axis_size(axis)
    before = lax.ppermute(forward, axis, [(i, (i + 1) % count) for i in range(count)])
    after = lax.ppermute(backward, axis, [(i, (i - 1) % count) for i in range(count)])
    return before, after


def swap_halo(forward, backward, axis):
    count = lax.axis_size(axis)
    odd = lax.axis_index(axis) % 2 == 1
    if count % 2:
        before, after = halo(forward, backward, axis)
        return jnp.where(odd, before, after), jnp.where(odd, after, before)
    near = lax.ppermute(jnp.where(odd, backward, forward), axis, [(i, i ^ 1) for i in range(count)])
    far = lax.ppermute(
        jnp.where(odd, forward, backward),
        axis,
        [(i, (i + (1 if i % 2 else -1)) % count) for i in range(count)],
    )
    return near, far


def open_halo(forward, backward, axis):
    count = lax.axis_size(axis)
    index = lax.axis_index(axis)
    before, after = halo(forward, backward, axis)
    zero = jnp.zeros((), before.dtype)
    return jnp.where(index > 0, before, zero), jnp.where(index < count - 1, after, zero)


def side_by_side(values):
    rows = values.shape[0] // 2
    return jnp.concatenate([values[:rows], values[rows:]], axis=1)


def halve(block, axes, bit, dim=0):
    count = math.prod(lax.axis_size(axis) for axis in axes)
    index = lax.axis_index(axes)
    pairs = block.shape[:dim] + ((-1, 2) if block.shape[dim] > 2 else (2,))
    split = block.reshape(pairs + block.shape[dim + 1 :])
    dim = len(pairs) - 1
    mine = (index // bit) % 2
    keep = lax.dynamic_index_in_dim(split, mine, dim, keepdims=False)
    send = lax.dynamic_index_in_dim(split, 1 - mine, dim, keepdims=False)
    got = lax.ppermute(send, axes, [(i, i ^ bit) for i in range(count)])
    return keep.astype(F32) + got.astype(F32)


def halve_all(block, axes, bit=1):
    count = block.shape[0]
    while count > 1:
        block = halve(block.astype(BF16), axes, bit)
        bit, count = 2 * bit, count // 2
    return block


def window(
    fields, grain_ids, material_table, input_weight, kernel_fine, kernel_down, kernel_bottle,
    cotangent,
):
    comps, bx, by, bz = fields.shape
    grains, c1 = material_table.shape
    c2 = kernel_down.shape[0]
    outs_true = kernel_bottle.shape[0]
    gx, gy, gz = lax.axis_size("gx"), lax.axis_size("gy"), lax.axis_size("gz")
    nx, total_y, total_z = bx * gx, by * gy, bz * gz
    coarse_x = nx // 2
    nq = -(-(bz + 12) // 32) * 8
    outs = -(-outs_true // 128) * 128
    if outs != outs_true:
        kernel_bottle = jnp.pad(kernel_bottle, ((0, outs - outs_true), (0, 0)))
        cotangent = jnp.pad(cotangent, ((0, outs - outs_true), (0, 0), (0, 0), (0, 0)))

    quad = comps + 1
    half_y, half_z = by // 2, bz // 2
    vmem = pl.BlockSpec(memory_space=pltpu.VMEM)
    cot = jnp.transpose(cotangent, (1, 2, 3, 0))
    feat, cot = pl.pallas_call(
        pack_kernel,
        out_shape=(
            jax.ShapeDtypeStruct((bx * by, bz * quad), BF16),
            jax.ShapeDtypeStruct((math.prod(cot.shape[:3]), outs), BF16),
        ),
        in_specs=[vmem] * 3,
        out_specs=(vmem,) * 2,
        compiler_params=pltpu.CompilerParams(vmem_limit_bytes=4 << 20),
        name="pack",
    )(fields, grain_ids, cot.reshape(-1, outs))
    cot = cot.reshape(coarse_x, half_y, half_z, outs)
    feat = lax.all_gather(feat.reshape(bx, by, bz * quad), "gx", axis=0, tiled=True)

    def packed(first, second):
        return jnp.concatenate([first.reshape(-1, 128), second.reshape(-1, 128)], axis=0)

    def unpacked(both, first_shape, second_shape):
        cut = math.prod(first_shape) // 128
        return both[:cut].reshape(first_shape), both[cut:].reshape(second_shape)

    before, after = open_halo(
        packed(feat[:, by - 6 :], cot[:, half_y - 1 :]), packed(feat[:, :5], cot[:, :1]), "gy"
    )
    edge = (coarse_x, 1, half_z, outs)
    feat_before, cot_before = unpacked(before, (nx, 6, bz * quad), edge)
    feat_after, cot_after = unpacked(after, (nx, 5, bz * quad), edge)
    feat = jnp.concatenate([feat_before, feat, feat_after], axis=1)
    cot = jnp.concatenate([cot_before, cot, cot_after], axis=1)
    near, far = swap_halo(
        packed(feat, cot[:, :, half_z - 1 :]), packed(feat, cot[:, :, :1]), "gz"
    )
    wide_weight, wide_table = pl.pallas_call(
        widen_inputs,
        out_shape=(
            jax.ShapeDtypeStruct((4 * quad, 4 * c1), F32),
            jax.ShapeDtypeStruct((4 * grains, 4 * c1), BF16),
        ),
        in_specs=[vmem] * 2,
        out_specs=(vmem,) * 2,
        compiler_params=pltpu.CompilerParams(vmem_limit_bytes=4 << 20),
        name="widen",
    )(input_weight.T, material_table.T)
    place = jnp.stack([lax.axis_index("gy"), lax.axis_index("gz"), lax.axis_index("gx")])

    ny_own, ny_mid, ny_bot = by // 2, by // 2 + 4, by // 2 + 2
    own_x = bx // 2
    lanes = 6 * c1
    own_rows = own_x * ny_own * nq
    kept = (own_x + 1, 2, ny_own + 1, 2, nq, lanes)
    limit = min(60 << 20, (14 << 20) + nx * (5 << 17))
    bottle_rows, mine, others, bottle_part, slope, fine_own = pl.pallas_call(
        lambda *refs: forward_kernel(
            *refs, dims=(nx, by, bz, c1, c2, outs, grains, (total_y, total_z))
        ),
        out_shape=(
            jax.ShapeDtypeStruct((coarse_x * ny_own * nq, 2 * outs), BF16),
            jax.ShapeDtypeStruct((own_rows, 2 * c2), BF16),
            jax.ShapeDtypeStruct((gx - 1, own_rows, 2 * c2), BF16),
            jax.ShapeDtypeStruct((27 * c2, outs), BF16),
            jax.ShapeDtypeStruct((own_x * ny_own * nq, 2 * c2), F32),
            jax.ShapeDtypeStruct((math.prod(kept[:-1]), lanes), BF16),
        ),
        in_specs=[pl.BlockSpec(memory_space=pltpu.SMEM)] + [vmem] * 9,
        out_specs=(vmem,) * 6,
        scratch_shapes=[
            pltpu.VMEM((lanes // LANES, (nx + 2) * (by + 11) * nq, LANES), F32),
            pltpu.VMEM((coarse_x + 1, 2, (by + 10) // 2, 2, nq, lanes), F32),
            pltpu.VMEM((coarse_x + 2, ny_mid, nq, 4 * c2), F32),
            pltpu.VMEM((coarse_x + 2, ny_bot, nq, 4 * outs), F32),
            pltpu.VMEM((coarse_x, ny_mid, nq, 2 * c2), F32),
            pltpu.VMEM(((by + 9) * nq, 4 * c1), F32),
            pltpu.VMEM((ny_mid * nq, 2 * c2), F32),
            pltpu.VMEM((nx * (by + 11), 4 * nq * quad), F32),
            pltpu.VMEM((outs // LANES, coarse_x * ny_bot * bz // 2, LANES), F32),
            pltpu.VMEM((2 * outs // LANES, coarse_x * ny_bot * nq, LANES), F32),
            pltpu.VMEM((9 * lanes, 4 * c1), BF16),
            pltpu.VMEM((9 * 4 * c1, c2), BF16),
        ],
        compiler_params=pltpu.CompilerParams(vmem_limit_bytes=limit),
        cost_estimate=pl.CostEstimate(flops=10**10, transcendentals=0, bytes_accessed=10**7),
        name="forward",
    )(
        place, feat.reshape(-1, bz * quad), near, far, cot.reshape(-1, outs),
        wide_weight, wide_table, kernel_fine, kernel_down.T, kernel_bottle,
    )

    bottle = bottle_rows.reshape(coarse_x, ny_own, 2 * nq, outs)[:, :, 2 : 2 + bz // 2]
    bottle = jnp.transpose(bottle, (3, 0, 1, 2))[:outs_true]

    other = jnp.stack(
        [
            lax.ppermute(others[k - 1], "gx", [(i, (i + k) % gx) for i in range(gx)])
            for k in range(1, gx)
        ]
    )

    chunks = gy * gz
    rows = 27 * c1 // chunks
    paired = gx == 2 and rows % 2 == 0 and chunks % 8 == 0
    part_shape = (chunks, 2, rows // 2, c2) if paired else (27 * c1, c2)
    scale = 1.0 / math.sqrt(coarse_x * (total_y // 2) * (total_z // 2))
    down_part = pl.pallas_call(
        lambda *refs: down_kernel(*refs, dims=(bz, c1, c2, nq, scale)),
        out_shape=jax.ShapeDtypeStruct(part_shape, BF16),
        in_specs=[vmem] * 4,
        out_specs=vmem,
        scratch_shapes=[
            pltpu.VMEM((27 * c1, c2), F32),
            pltpu.VMEM(kept, F32),
        ],
        compiler_params=pltpu.CompilerParams(vmem_limit_bytes=10 << 20),
        cost_estimate=pl.CostEstimate(flops=2 * 10**9, transcendentals=0, bytes_accessed=10**6),
        name="down_gradient",
    )(mine, other, slope, fine_own)

    both = ("gy", "gz")
    bottle_part = bottle_part.reshape(chunks, 27 * c2 // chunks, outs)
    if paired:
        bottle_part = halve(bottle_part, both, 1).astype(BF16)
        bottle_part = halve(bottle_part, both, 2).astype(BF16)
        down_part = halve(down_part, both, 1).astype(BF16)
        down_part = halve(down_part, ("gx",), 1, 1).astype(BF16)
        down_part = halve(down_part, both, 2).astype(BF16)
        joined = jnp.concatenate([bottle_part, down_part], axis=1)
        cut = bottle_part.shape[1]
        bit = 4
        while joined.shape[0] > 2:
            joined = halve(joined, both, bit).astype(BF16)
            bit *= 2
        mine = (lax.axis_index(both) // bit) % 2
        send = lax.dynamic_index_in_dim(joined, 1 - mine, 0, keepdims=False)
        got = lax.ppermute(send, both, [(i, i ^ bit) for i in range(chunks)])
        grad_bottle, grad_down = pl.pallas_call(
            finish_kernel,
            out_shape=(
                jax.ShapeDtypeStruct((cut, outs), F32),
                jax.ShapeDtypeStruct((c2 // 2, rows), F32),
            ),
            in_specs=[pl.BlockSpec(memory_space=pltpu.SMEM)] + [vmem] * 2,
            out_specs=(vmem,) * 2,
            compiler_params=pltpu.CompilerParams(vmem_limit_bytes=4 << 20),
            name="finish",
        )(mine.reshape(1), joined, got)
        grad_bottle = grad_bottle[:, :outs_true].T
    else:
        grad_bottle = halve_all(bottle_part, both)[:, :outs_true].T
        down_part = jnp.transpose(down_part.reshape(27 * c1, gx, c2 // gx), (1, 0, 2))
        down_part = halve_all(down_part, ("gx",)).reshape(chunks, rows, c2 // gx)
        grad_down = halve_all(down_part, both).T
    return (bottle, grad_down, grad_bottle)


def solution(mesh):
    placed = (
        P(None, "gx", "gy", "gz"),
        P("gx", "gy", "gz"),
        P(),
        P(),
        P(),
        P(),
        P("gx", None),
        P("gx", None, "gy", "gz"),
    )
    return jax.shard_map(
        window,
        mesh=mesh,
        in_specs=placed,
        out_specs=(P("gx", None, "gy", "gz"), P("gx", ("gy", "gz")), P("gx", ("gy", "gz"))),
        check_vma=False,
    )
```

```python
import math

import jax
import jax.numpy as jnp
from jax import lax
from jax.experimental import pallas as pl
from jax.experimental.pallas import tpu as pltpu
from jax.sharding import PartitionSpec as P

F32 = jnp.float32
BF16 = jnp.bfloat16
CONTRACT_LANES = (((1,), (1,)), ((), ()))
CONTRACT_PLAIN = (((1,), (0,)), ((), ()))
LANES = 128
FINE_STEP = 8
MID_STEP = 4
TAPS_XY = [(kx, ky) for kx in range(3) for ky in range(3)]


def silu(values):
    half = 0.5 * values
    return half + half * jnp.tanh(half)


def silu_grad(values):
    sigmoid = 0.5 + 0.5 * jnp.tanh(0.5 * values)
    return sigmoid * (1.0 + values * (1.0 - sigmoid))


def flat(values):
    return values.reshape(-1, values.shape[-1])


def next_row(values):
    return pltpu.roll(values, values.shape[0] - 1, 0)


def previous_row(values):
    return pltpu.roll(values, 1, 0)


def pack_kernel(fields, grain_ids, cotangent, out, cot_out):
    comps, bx, by, bz = fields.shape
    quad = comps + 1
    column = lax.broadcasted_iota(jnp.int32, (bz, bz * quad), 1)
    row = lax.broadcasted_iota(jnp.int32, (bz, bz * quad), 0)
    total = jnp.zeros((bx * by, bz * quad), F32)
    for c in range(quad):
        plane = fields[c].astype(F32) if c < comps else (grain_ids[...] + 1).astype(F32)
        spread = jnp.where(column == row * quad + c, 1.0, 0.0).astype(BF16)
        total = total + jnp.dot(flat(plane).astype(BF16), spread, preferred_element_type=F32)
    out[...] = total.astype(BF16)
    cot_out[...] = cotangent[...]


def widen_inputs(weight, table, weight_out, table_out):
    comps, c1 = weight.shape
    grains = table.shape[1]
    quad = comps + 1
    weight_out[...] = jnp.zeros(weight_out.shape, F32)
    table_out[...] = jnp.zeros(table_out.shape, BF16)
    entries = jnp.transpose(table[...].astype(F32), (1, 0)).astype(BF16)
    for k in range(4):
        weight_out[k * quad : k * quad + comps, k * c1 : (k + 1) * c1] = weight[...].astype(F32)
        table_out[k * grains : (k + 1) * grains, k * c1 : (k + 1) * c1] = entries


def widen_kernels(kernel_fine, kernel_down, fine_out, down_out):
    c1 = kernel_fine.shape[0]
    width = 3 * c1
    turned = jnp.transpose(kernel_fine[...].astype(F32), (1, 0))
    fine_out[...] = jnp.zeros(fine_out.shape, BF16)
    for tap in range(9):
        piece = turned[tap * width : (tap + 1) * width].astype(BF16)
        for k in range(4):
            start = tap * 2 * width + k * c1
            fine_out[start : start + width, k * c1 : (k + 1) * c1] = piece
        start = tap * 4 * c1
        down_out[start : start + width, :] = kernel_down[tap * width : (tap + 1) * width, :]
        down_out[start + width : start + 4 * c1, :] = jnp.zeros((c1, down_out.shape[1]), BF16)


def forward_kernel(
    place, feat, near, far, cot, wide_weight, wide_table, kernel_fine, kernel_down, kernel_bottle,
    bottle_out, mine_out, others_out, grad_out, slope_out, kept_out,
    emb, fine, coarse, grads, pre, fine_mask, coarse_mask, wide_feat, cot_rows, cotangent,
    band_fine, band_down, *, dims,
):
    nx, by, bz, c1, c2, outs, grains, limits = dims
    total_y, total_z = limits
    ny_emb, ny_fine, ny_mid, ny_bot, ny_own = by + 11, by + 9, by // 2 + 4, by // 2 + 2, by // 2
    quad = wide_weight.shape[0] // 4
    nq = fine.shape[4]
    coarse_x = nx // 2
    own_x = slope_out.shape[0] // (ny_own * nq)
    groups = coarse_x // own_x
    lanes = 4 * c1
    half = lanes // 2
    half_z = bz // 2


    emb_rows = nx * ny_emb
    has_before = place[1] > 0
    has_after = place[1] < total_z // bz - 1
    odd = place[1] % 2 == 1
    near_all, far_all = near[...].astype(F32), far[...].astype(F32)
    before = jnp.where(has_before, jnp.where(odd, near_all, far_all), 0.0)
    after = jnp.where(has_after, jnp.where(odd, far_all, near_all), 0.0)
    low, high = before[:emb_rows], after[:emb_rows]
    spare = jnp.zeros((emb_rows, 4 * nq * quad - (bz + 12) * quad), F32)
    wide_feat[...] = jnp.concatenate(
        [low[:, (bz - 6) * quad :], feat[...].astype(F32), high[:, : 6 * quad], spare], axis=1
    )
    columns = coarse_x * ny_bot
    cotangent[...] = jnp.zeros(cotangent.shape, F32)
    edge_low = before[emb_rows:].reshape(-1, outs)
    edge_high = after[emb_rows:].reshape(-1, outs)
    slabs = outs // LANES
    cot_wide = cot[...].astype(F32)
    for k in range(slabs):
        cot_rows[k] = cot_wide[:, k * LANES : (k + 1) * LANES]
        for z in range(half_z):
            target = (z % 2 * slabs + k, pl.ds(z // 2 + 1, columns, stride=nq))
            cotangent[target] = cot_rows[k, pl.ds(z, columns, stride=half_z)]
        cotangent[slabs + k, pl.ds(0, columns, stride=nq)] = edge_low[:, k * LANES : (k + 1) * LANES]
        cotangent[k, pl.ds(half_z // 2 + 1, columns, stride=nq)] = edge_high[:, k * LANES : (k + 1) * LANES]

    shape = (ny_fine * nq, lanes)
    row = lax.broadcasted_iota(jnp.int32, shape, 0)
    lane = lax.broadcasted_iota(jnp.int32, shape, 1)
    y = place[0] * by - 5 + row // nq
    z = place[1] * bz - 5 + 4 * (row % nq) + lane // c1
    inside = (y >= 0) & (y < total_y) & (z >= 0) & (z < total_z)
    fine_mask[...] = jnp.where(inside, 1.0, 0.0)
    shape = (ny_mid * nq, 2 * c2)
    row = lax.broadcasted_iota(jnp.int32, shape, 0)
    lane = lax.broadcasted_iota(jnp.int32, shape, 1)
    y = place[0] * (by // 2) - 2 + row // nq
    z = place[1] * (bz // 2) - 2 + 2 * (row % nq) + lane // c2
    inside = (y >= 0) & (y < total_y // 2) & (z >= 0) & (z < total_z // 2)
    coarse_mask[...] = jnp.where(inside, 1.0, 0.0)

    layer_rows = ny_emb * nq
    blank = jnp.zeros((emb.shape[0], layer_rows, LANES), F32)
    emb[:, :layer_rows] = blank
    emb[:, (nx + 1) * layer_rows :] = blank
    fine[0, 0] = jnp.zeros(fine.shape[2:], F32)
    coarse[0] = jnp.zeros(coarse.shape[1:], F32)
    coarse[coarse_x + 1] = jnp.zeros(coarse.shape[1:], F32)
    grads[0] = jnp.zeros(grads.shape[1:], F32)
    grads[coarse_x + 1] = jnp.zeros(grads.shape[1:], F32)

    emb_step = 8
    chunk = emb_step * ny_emb

    def embed(step, carry):
        start = pl.multiple_of(step * chunk, 8)
        values = wide_feat[pl.ds(start, chunk), :]
        grain = lax.broadcasted_iota(jnp.int32, (1, grains), 1).astype(F32) + 1.0
        base = start * nq + layer_rows
        for q in range(nq):
            part = values[:, 4 * quad * q : 4 * quad * (q + 1)]
            picks = [
                jnp.where(part[:, quad * k + quad - 1 : quad * k + quad] == grain, 1.0, 0.0)
                for k in range(4)
            ]
            picks = jnp.concatenate([pick.astype(BF16) for pick in picks], axis=1)
            mixture = jnp.dot(
                part.astype(BF16), wide_weight[...].astype(BF16), preferred_element_type=F32
            ) + jnp.dot(picks, wide_table[...], preferred_element_type=F32)
            out = silu(mixture).astype(BF16).astype(F32)
            following = out[:, :half] if q else jnp.zeros((chunk, half), F32)
            for k in range(lanes // LANES):
                target = (k, pl.ds(base + q, chunk, stride=nq))
                emb[target] = out[:, k * LANES : (k + 1) * LANES]
            for k in range(half // LANES):
                target = (lanes // LANES + k, pl.ds(base + (q - 1) % nq, chunk, stride=nq))
                emb[target] = following[:, k * LANES : (k + 1) * LANES]
        return carry

    lax.fori_loop(0, nx // emb_step, embed, 0)

    widen_kernels(kernel_fine, kernel_down, band_fine, band_down)

    fine_step = FINE_STEP

    def fine_conv(step, carry):
        x0 = step * fine_step

        def layers(kx, ky):
            pieces = []
            for i in range(fine_step):
                start = pl.multiple_of((x0 + i + kx) * layer_rows + ky * nq, 8)
                pieces.append(
                    jnp.concatenate(
                        [emb[k, pl.ds(start, ny_fine * nq)] for k in range(emb.shape[0])], axis=1
                    )
                )
            return jnp.concatenate(pieces, axis=0).astype(BF16)

        patches = jnp.concatenate([layers(kx, ky) for kx, ky in TAPS_XY], axis=1)
        values = lax.dot_general(
            patches, band_fine[...], CONTRACT_PLAIN, preferred_element_type=F32
        )
        rows = ny_fine * nq
        for i in range(fine_step):
            layer = silu(values[i * rows : (i + 1) * rows]) * fine_mask[...]
            layer = layer.astype(BF16).astype(F32)
            following = next_row(layer[:, :half])
            for j in range(ny_fine):
                target = (x0 // 2 + (1 + i) // 2, (1 + i) % 2, j // 2, j % 2)
                fine[target + (slice(None), slice(0, lanes))] = layer[j * nq : (j + 1) * nq]
                fine[target + (slice(None), slice(lanes, None))] = following[j * nq : (j + 1) * nq]
        return carry

    lax.fori_loop(0, nx // fine_step, fine_conv, 0)

    first = place[2] * own_x
    kept_out[...] = flat(fine[pl.ds(first, own_x + 1), :, 2 : 3 + ny_own]).astype(BF16)

    mid_step = MID_STEP if coarse_x % MID_STEP == 0 else own_x

    def down_conv(step, carry):
        x0 = step * mid_step
        taps = [
            flat(
                fine[pl.ds(x0 + kx // 2, mid_step), kx % 2, ky // 2 : ky // 2 + ny_mid, ky % 2]
            ).astype(BF16)
            for kx, ky in TAPS_XY
        ]
        patches = jnp.concatenate(
            [
                jnp.concatenate([tap[:, 2 * k * c1 : 2 * k * c1 + lanes] for tap in taps], axis=1)
                for k in range(2)
            ],
            axis=0,
        )
        values = side_by_side(
            lax.dot_general(patches, band_down[...], CONTRACT_PLAIN, preferred_element_type=F32)
        )
        pre[pl.ds(x0, mid_step)] = values.reshape(mid_step, ny_mid, nq, 2 * c2)
        inside = coarse_mask[...]
        inside = jnp.concatenate([inside] * mid_step, axis=0)
        act = (silu(values) * inside).astype(BF16).astype(F32)
        where = pl.ds(1 + x0, mid_step)
        whole = (mid_step, ny_mid, nq)
        coarse[where, :, :, :c2] = previous_row(act[:, c2:]).reshape(whole + (c2,))
        coarse[where, :, :, c2 : 3 * c2] = act.reshape(whole + (2 * c2,))
        coarse[where, :, :, 3 * c2 :] = next_row(act[:, :c2]).reshape(whole + (c2,))
        return carry

    lax.fori_loop(0, coarse_x // mid_step, down_conv, 0)

    bot_rows = ny_bot * nq

    def bottle_conv(step, carry):
        x0 = step * mid_step
        taps = [
            flat(coarse[pl.ds(x0 + kx, mid_step), ky : ky + ny_bot]).astype(BF16)
            for kx, ky in TAPS_XY
        ]
        patches = jnp.concatenate(
            [
                jnp.concatenate([tap[:, k * c2 : (k + 3) * c2] for tap in taps], axis=1)
                for k in range(2)
            ],
            axis=0,
        )
        values = side_by_side(
            lax.dot_general(
                patches, kernel_bottle[...], CONTRACT_LANES, preferred_element_type=F32
            )
        )
        start = pl.multiple_of(x0 * bot_rows, 8)
        spread = [
            cotangent[k, pl.ds(start, mid_step * bot_rows)] for k in range(cotangent.shape[0])
        ]
        grad = jnp.concatenate(spread, axis=1) * silu_grad(values)
        grad = grad.astype(BF16).astype(F32)
        where = pl.ds(1 + x0, mid_step)
        whole = (mid_step, ny_bot, nq)
        grads[where, :, :, :outs] = previous_row(grad[:, outs:]).reshape(whole + (outs,))
        grads[where, :, :, outs : 3 * outs] = grad.reshape(whole + (2 * outs,))
        grads[where, :, :, 3 * outs :] = next_row(grad[:, :outs]).reshape(whole + (outs,))
        act = silu(values).reshape(whole + (2 * outs,))[:, 1 : 1 + ny_own]
        start = pl.multiple_of(x0 * ny_own * nq, 16)
        bottle_out[pl.ds(start, mid_step * ny_own * nq), :] = flat(act).astype(BF16)
        return carry

    lax.fori_loop(0, coarse_x // mid_step, bottle_conv, 0)

    stacked = jnp.concatenate(
        [kernel_bottle[:, t * c2 : (t + 1) * c2] for t in range(27)], axis=0
    )
    own_rows = ny_own * nq

    def transpose_conv(step, carry):
        x0 = step * mid_step
        taps = [
            flat(grads[pl.ds(x0 + 2 - kx, mid_step), 2 - ky : 2 - ky + ny_own]).astype(BF16)
            for kx, ky in TAPS_XY
        ]
        patches = jnp.concatenate(
            [
                jnp.concatenate(
                    [
                        tap[:, (k + 2 - kz) * outs : (k + 3 - kz) * outs]
                        for tap in taps
                        for kz in range(3)
                    ],
                    axis=1,
                )
                for k in range(2)
            ],
            axis=0,
        )
        values = side_by_side(
            lax.dot_general(patches, stacked, CONTRACT_PLAIN, preferred_element_type=F32)
        )
        values = values.astype(BF16)
        for k in range(mid_step // own_x):
            piece = values[k * own_x * own_rows : (k + 1) * own_x * own_rows]
            owner = lax.rem(x0 // own_x + k - place[2] + groups, groups)

            @pl.when(owner == 0)
            def _(piece=piece):
                mine_out[...] = piece

            @pl.when(owner > 0)
            def _(piece=piece, owner=owner):
                others_out[owner - 1] = piece

        return carry

    lax.fori_loop(0, coarse_x // mid_step, transpose_conv, 0)

    scale = 1.0 / math.sqrt(coarse_x * (total_y // 2) * (total_z // 2))
    own = flat(grads[1 : 1 + coarse_x, 1 : 1 + ny_own, :, outs : 3 * outs])
    place_row = lax.broadcasted_iota(jnp.int32, own.shape, 0) % nq
    own = jnp.where((place_row >= 1) & (place_row <= bz // 4), own, 0.0)
    turned = jnp.transpose(own, (1, 0)).astype(BF16)
    for number, (kx, ky) in enumerate(TAPS_XY):
        rows = flat(coarse[kx : kx + coarse_x, ky + 1 : ky + 1 + ny_own]).astype(BF16)
        product = jnp.dot(turned, rows, preferred_element_type=F32)
        total = product[:outs, : 3 * c2] + product[outs:, c2:]
        total = jnp.transpose(total * scale, (1, 0)).astype(BF16)
        grad_out[number * 3 * c2 : (number + 1) * 3 * c2, :] = total

    slope = silu_grad(pre[pl.ds(first, own_x), 2 : 2 + ny_own])
    slope_out[...] = flat(slope)


def down_kernel(mine, other, slope, kept, grad_out, total_ref, fine, *, dims):
    bz, c1, c2, nq, scale = dims
    own_x, ny_own = fine.shape[0] - 1, fine.shape[2] - 1
    grad = jnp.sum(other[...].astype(F32), axis=0) + mine[...].astype(F32)
    grad = (grad * slope[...]).astype(BF16).astype(F32)
    place_row = lax.broadcasted_iota(jnp.int32, grad.shape, 0) % nq
    grad = jnp.where((place_row >= 1) & (place_row <= bz // 4), grad, 0.0)
    turned = jnp.transpose(grad, (1, 0)).astype(BF16)
    fine[...] = kept[...].astype(F32).reshape(fine.shape)
    for number, (kx, ky) in enumerate(TAPS_XY):
        rows = flat(
            fine[kx // 2 : kx // 2 + own_x, kx % 2, ky // 2 : ky // 2 + ny_own, ky % 2]
        ).astype(BF16)
        product = jnp.dot(turned, rows, preferred_element_type=F32)
        total = product[:c2, : 4 * c1] + product[c2:, 2 * c1 : 6 * c1]
        total = jnp.transpose(total * scale, (1, 0))[: 3 * c1]
        total_ref[number * 3 * c1 : (number + 1) * 3 * c1, :] = total
    if len(grad_out.shape) == 2:
        grad_out[...] = total_ref[...].astype(BF16)
        return
    chunks, rows = grad_out.shape[0], grad_out.shape[2]
    low = lax.broadcasted_iota(jnp.int32, (rows, c2), 1) < c2 // 2
    for k in range(chunks):
        first = total_ref[2 * k * rows : (2 * k + 1) * rows, :]
        second = total_ref[(2 * k + 1) * rows : (2 * k + 2) * rows, :]
        grad_out[k, 0] = jnp.where(low, first, pltpu.roll(second, c2 // 2, 1)).astype(BF16)
        grad_out[k, 1] = jnp.where(low, pltpu.roll(first, c2 // 2, 1), second).astype(BF16)


def finish_kernel(index, joined, got, bottle_out, down_out):
    cut = bottle_out.shape[0]
    width = down_out.shape[0]
    total = joined[index[0]].astype(F32) + got[...].astype(F32)
    bottle_out[...] = total[:cut]
    turned = jnp.transpose(total[cut:], (1, 0))
    down_out[...] = jnp.concatenate([turned[:width], turned[width:]], axis=1)


def halo(forward, backward, axis):
    count = lax.axis_size(axis)
    before = lax.ppermute(forward, axis, [(i, (i + 1) % count) for i in range(count)])
    after = lax.ppermute(backward, axis, [(i, (i - 1) % count) for i in range(count)])
    return before, after


def swap_halo(forward, backward, axis):
    count = lax.axis_size(axis)
    odd = lax.axis_index(axis) % 2 == 1
    if count % 2:
        before, after = halo(forward, backward, axis)
        return jnp.where(odd, before, after), jnp.where(odd, after, before)
    near = lax.ppermute(jnp.where(odd, backward, forward), axis, [(i, i ^ 1) for i in range(count)])
    far = lax.ppermute(
        jnp.where(odd, forward, backward),
        axis,
        [(i, (i + (1 if i % 2 else -1)) % count) for i in range(count)],
    )
    return near, far


def open_halo(forward, backward, axis):
    count = lax.axis_size(axis)
    index = lax.axis_index(axis)
    before, after = halo(forward, backward, axis)
    zero = jnp.zeros((), before.dtype)
    return jnp.where(index > 0, before, zero), jnp.where(index < count - 1, after, zero)


def side_by_side(values):
    rows = values.shape[0] // 2
    return jnp.concatenate([values[:rows], values[rows:]], axis=1)


def halve(block, axes, bit, dim=0):
    count = math.prod(lax.axis_size(axis) for axis in axes)
    index = lax.axis_index(axes)
    pairs = block.shape[:dim] + ((-1, 2) if block.shape[dim] > 2 else (2,))
    split = block.reshape(pairs + block.shape[dim + 1 :])
    dim = len(pairs) - 1
    mine = (index // bit) % 2
    keep = lax.dynamic_index_in_dim(split, mine, dim, keepdims=False)
    send = lax.dynamic_index_in_dim(split, 1 - mine, dim, keepdims=False)
    got = lax.ppermute(send, axes, [(i, i ^ bit) for i in range(count)])
    return keep.astype(F32) + got.astype(F32)


def halve_all(block, axes, bit=1):
    count = block.shape[0]
    while count > 1:
        block = halve(block.astype(BF16), axes, bit)
        bit, count = 2 * bit, count // 2
    return block


def window(
    fields, grain_ids, material_table, input_weight, kernel_fine, kernel_down, kernel_bottle,
    cotangent,
):
    comps, bx, by, bz = fields.shape
    grains, c1 = material_table.shape
    c2 = kernel_down.shape[0]
    outs_true = kernel_bottle.shape[0]
    gx, gy, gz = lax.axis_size("gx"), lax.axis_size("gy"), lax.axis_size("gz")
    nx, total_y, total_z = bx * gx, by * gy, bz * gz
    coarse_x = nx // 2
    nq = -(-(bz + 12) // 32) * 8
    outs = -(-outs_true // 128) * 128
    if outs != outs_true:
        kernel_bottle = jnp.pad(kernel_bottle, ((0, outs - outs_true), (0, 0)))
        cotangent = jnp.pad(cotangent, ((0, outs - outs_true), (0, 0), (0, 0), (0, 0)))

    quad = comps + 1
    half_y, half_z = by // 2, bz // 2
    vmem = pl.BlockSpec(memory_space=pltpu.VMEM)
    cot = jnp.transpose(cotangent, (1, 2, 3, 0))
    feat, cot = pl.pallas_call(
        pack_kernel,
        out_shape=(
            jax.ShapeDtypeStruct((bx * by, bz * quad), BF16),
            jax.ShapeDtypeStruct((math.prod(cot.shape[:3]), outs), BF16),
        ),
        in_specs=[vmem] * 3,
        out_specs=(vmem,) * 2,
        compiler_params=pltpu.CompilerParams(vmem_limit_bytes=4 << 20),
        name="pack",
    )(
        *(
            pltpu.with_memory_space_constraint(x, pltpu.HBM)
            for x in (fields, grain_ids, cot.reshape(-1, outs))
        )
    )
    cot = cot.reshape(coarse_x, half_y, half_z, outs)
    feat = lax.all_gather(feat.reshape(bx, by, bz * quad), "gx", axis=0, tiled=True)

    def packed(first, second):
        return jnp.concatenate([first.reshape(-1, 128), second.reshape(-1, 128)], axis=0)

    def unpacked(both, first_shape, second_shape):
        cut = math.prod(first_shape) // 128
        return both[:cut].reshape(first_shape), both[cut:].reshape(second_shape)

    before, after = open_halo(
        packed(feat[:, by - 6 :], cot[:, half_y - 1 :]), packed(feat[:, :5], cot[:, :1]), "gy"
    )
    edge = (coarse_x, 1, half_z, outs)
    feat_before, cot_before = unpacked(before, (nx, 6, bz * quad), edge)
    feat_after, cot_after = unpacked(after, (nx, 5, bz * quad), edge)
    feat = jnp.concatenate([feat_before, feat, feat_after], axis=1)
    cot = jnp.concatenate([cot_before, cot, cot_after], axis=1)
    near, far = swap_halo(
        packed(feat, cot[:, :, half_z - 1 :]), packed(feat, cot[:, :, :1]), "gz"
    )
    wide_weight, wide_table = pl.pallas_call(
        widen_inputs,
        out_shape=(
            jax.ShapeDtypeStruct((4 * quad, 4 * c1), F32),
            jax.ShapeDtypeStruct((4 * grains, 4 * c1), BF16),
        ),
        in_specs=[vmem] * 2,
        out_specs=(vmem,) * 2,
        compiler_params=pltpu.CompilerParams(vmem_limit_bytes=4 << 20),
        name="widen",
    )(input_weight.T, material_table.T)
    place = jnp.stack([lax.axis_index("gy"), lax.axis_index("gz"), lax.axis_index("gx")])

    ny_own, ny_mid, ny_bot = by // 2, by // 2 + 4, by // 2 + 2
    own_x = bx // 2
    lanes = 6 * c1
    own_rows = own_x * ny_own * nq
    kept = (own_x + 1, 2, ny_own + 1, 2, nq, lanes)
    limit = min(60 << 20, (14 << 20) + nx * (5 << 17))
    bottle_rows, mine, others, bottle_part, slope, fine_own = pl.pallas_call(
        lambda *refs: forward_kernel(
            *refs, dims=(nx, by, bz, c1, c2, outs, grains, (total_y, total_z))
        ),
        out_shape=(
            jax.ShapeDtypeStruct((coarse_x * ny_own * nq, 2 * outs), BF16),
            jax.ShapeDtypeStruct((own_rows, 2 * c2), BF16),
            jax.ShapeDtypeStruct((gx - 1, own_rows, 2 * c2), BF16),
            jax.ShapeDtypeStruct((27 * c2, outs), BF16),
            jax.ShapeDtypeStruct((own_x * ny_own * nq, 2 * c2), F32),
            jax.ShapeDtypeStruct((math.prod(kept[:-1]), lanes), BF16),
        ),
        in_specs=[pl.BlockSpec(memory_space=pltpu.SMEM)] + [vmem] * 9,
        out_specs=(vmem,) * 6,
        scratch_shapes=[
            pltpu.VMEM((lanes // LANES, (nx + 2) * (by + 11) * nq, LANES), F32),
            pltpu.VMEM((coarse_x + 1, 2, (by + 10) // 2, 2, nq, lanes), F32),
            pltpu.VMEM((coarse_x + 2, ny_mid, nq, 4 * c2), F32),
            pltpu.VMEM((coarse_x + 2, ny_bot, nq, 4 * outs), F32),
            pltpu.VMEM((coarse_x, ny_mid, nq, 2 * c2), F32),
            pltpu.VMEM(((by + 9) * nq, 4 * c1), F32),
            pltpu.VMEM((ny_mid * nq, 2 * c2), F32),
            pltpu.VMEM((nx * (by + 11), 4 * nq * quad), F32),
            pltpu.VMEM((outs // LANES, coarse_x * ny_bot * bz // 2, LANES), F32),
            pltpu.VMEM((2 * outs // LANES, coarse_x * ny_bot * nq, LANES), F32),
            pltpu.VMEM((9 * lanes, 4 * c1), BF16),
            pltpu.VMEM((9 * 4 * c1, c2), BF16),
        ],
        compiler_params=pltpu.CompilerParams(vmem_limit_bytes=limit),
        cost_estimate=pl.CostEstimate(flops=10**10, transcendentals=0, bytes_accessed=10**7),
        name="forward",
    )(
        place, feat.reshape(-1, bz * quad), near, far, cot.reshape(-1, outs),
        wide_weight, wide_table, kernel_fine, kernel_down.T, kernel_bottle,
    )

    bottle = bottle_rows.reshape(coarse_x, ny_own, 2 * nq, outs)[:, :, 2 : 2 + bz // 2]
    bottle = jnp.transpose(bottle, (3, 0, 1, 2))[:outs_true]

    other = jnp.stack(
        [
            lax.ppermute(others[k - 1], "gx", [(i, (i + k) % gx) for i in range(gx)])
            for k in range(1, gx)
        ]
    )

    chunks = gy * gz
    rows = 27 * c1 // chunks
    paired = gx == 2 and rows % 2 == 0 and chunks % 8 == 0
    part_shape = (chunks, 2, rows // 2, c2) if paired else (27 * c1, c2)
    scale = 1.0 / math.sqrt(coarse_x * (total_y // 2) * (total_z // 2))
    down_part = pl.pallas_call(
        lambda *refs: down_kernel(*refs, dims=(bz, c1, c2, nq, scale)),
        out_shape=jax.ShapeDtypeStruct(part_shape, BF16),
        in_specs=[vmem] * 4,
        out_specs=vmem,
        scratch_shapes=[
            pltpu.VMEM((27 * c1, c2), F32),
            pltpu.VMEM(kept, F32),
        ],
        compiler_params=pltpu.CompilerParams(vmem_limit_bytes=10 << 20),
        cost_estimate=pl.CostEstimate(flops=2 * 10**9, transcendentals=0, bytes_accessed=10**6),
        name="down_gradient",
    )(mine, other, slope, fine_own)

    both = ("gy", "gz")
    bottle_part = bottle_part.reshape(chunks, 27 * c2 // chunks, outs)
    if paired:
        bottle_part = halve(bottle_part, both, 1).astype(BF16)
        bottle_part = halve(bottle_part, both, 2).astype(BF16)
        down_part = halve(down_part, both, 1).astype(BF16)
        down_part = halve(down_part, ("gx",), 1, 1).astype(BF16)
        down_part = halve(down_part, both, 2).astype(BF16)
        joined = jnp.concatenate([bottle_part, down_part], axis=1)
        cut = bottle_part.shape[1]
        bit = 4
        while joined.shape[0] > 2:
            joined = halve(joined, both, bit).astype(BF16)
            bit *= 2
        mine = (lax.axis_index(both) // bit) % 2
        send = lax.dynamic_index_in_dim(joined, 1 - mine, 0, keepdims=False)
        got = lax.ppermute(send, both, [(i, i ^ bit) for i in range(chunks)])
        grad_bottle, grad_down = pl.pallas_call(
            finish_kernel,
            out_shape=(
                jax.ShapeDtypeStruct((cut, outs), F32),
                jax.ShapeDtypeStruct((c2 // 2, rows), F32),
            ),
            in_specs=[pl.BlockSpec(memory_space=pltpu.SMEM)] + [vmem] * 2,
            out_specs=(vmem,) * 2,
            compiler_params=pltpu.CompilerParams(vmem_limit_bytes=4 << 20),
            name="finish",
        )(mine.reshape(1), joined, got)
        grad_bottle = grad_bottle[:, :outs_true].T
    else:
        grad_bottle = halve_all(bottle_part, both)[:, :outs_true].T
        down_part = jnp.transpose(down_part.reshape(27 * c1, gx, c2 // gx), (1, 0, 2))
        down_part = halve_all(down_part, ("gx",)).reshape(chunks, rows, c2 // gx)
        grad_down = halve_all(down_part, both).T
    return (bottle, grad_down, grad_bottle)


def solution(mesh):
    placed = (
        P(None, "gx", "gy", "gz"),
        P("gx", "gy", "gz"),
        P(),
        P(),
        P(),
        P(),
        P("gx", None),
        P("gx", None, "gy", "gz"),
    )
    return jax.shard_map(
        window,
        mesh=mesh,
        in_specs=placed,
        out_specs=(P("gx", None, "gy", "gz"), P("gx", ("gy", "gz")), P("gx", ("gy", "gz"))),
        check_vma=False,
    )
```
